512 devices in a mesh: ka: 32 (over x_lo, y, core), pb: 16 (over x_hi, z).
Axes of the slice: x: 4 (x_hi: 2, x_lo: 2; x = x_hi * 2 + x_lo), y: 8, z: 8, core: 2. Of those that a mesh axis runs over, the one named last changes fastest.
Arguments:
- targets: bfloat16 [32, 4, 2, 32768], P('ka'), may hold values from -6 to 6
- partners: bfloat16 [16, 2, 2, 32768], P('pb', None, None, 'ka'), may hold values from -6 to 6
- pair_map: int32 [32, 16], P('ka', 'pb'), may hold values from 0 to 63
- shifts: int32 [32, 16, 3], P('ka', 'pb'), may hold values from 0 to 1
Outputs:
- projector: float32 [32, 8, 2, 32768], P('ka', None, None, 'pb')
The draws below stay inside these ranges and needn't reach their ends.
Inputs may be any that keep to these rules, and one draw needn't show every extreme that they name: d = pair_map[k,q] names the mesh point (d // 16, (d // 4) mod 4, d mod 4).
All inputs are finite; a program needn't handle non-finite values.
Results may differ from the reference program's by a relative error of at most 0.015.
Values may be sent and summed in bfloat16 or wider, within the bound.
No kernel may reach another device: no remote copies, remote signals or barrier semaphores. Data moves between devices by JAX's collectives and lax.ppermute only.
A program may use at most 64 MiB of HBM per device.

```python
import jax
import jax.numpy as jnp
from jax import lax

GRID = 32
BANDS = 4
OCC = 2
NK = 32
NQ = 16


def touch_ends(entries, own_key, smallest, largest):
    index_at = [jax.random.randint(jax.random.fold_in(own_key, axis), (), 0, length) for axis, length in enumerate(entries.shape)]
    main_axis = entries.shape.index(max(entries.shape))
    next_to = index_at[:main_axis] + [(index_at[main_axis] + 1) % entries.shape[main_axis]] + index_at[main_axis + 1:]
    return entries.at[tuple(index_at)].set(smallest).at[tuple(next_to)].set(largest)


def shard_levels(rng, dims, pieces, least, top_value):
    gain = 1.0
    for axis_at, blocks in pieces:
        steps = jax.random.uniform(jax.random.fold_in(jax.random.fold_in(rng, 6), axis_at), (blocks,), jnp.float32, least / len(pieces), top_value / len(pieces))
        gain = gain * jnp.repeat(jnp.exp(steps), dims[axis_at] // blocks).reshape((-1,) + (1,) * (len(dims) - 1 - axis_at))
    return gain


def scatter_about(stream_key, shape, scale, limit, split=(), kind=jnp.bfloat16):
    gain = shard_levels(stream_key, shape, split, -0.22, 0.18) if split else 1.0
    values = jax.random.normal(stream_key, shape, jnp.float32) * scale * gain
    return jnp.minimum(jnp.maximum(values, -limit), limit).astype(kind)


def setup_inputs(seed: int = 0) -> dict:
    streams_of = jax.random.split(jax.random.key(seed), 5)
    targets = scatter_about(streams_of[0], (NK, BANDS, 2, GRID**3), 1.0, 6.0, ((0, 32),))
    partners = scatter_about(streams_of[1], (NQ, OCC, 2, GRID**3), 1.0, 6.0, ((0, 16), (3, 32)))
    pair_map = touch_ends(jax.random.randint(streams_of[2], (NK, NQ), 0, 64), jax.random.fold_in(streams_of[2], 1), 0, 63).astype(jnp.int32)
    shifts = touch_ends(jax.random.randint(streams_of[3], (NK, NQ, 3), 0, 2), jax.random.fold_in(streams_of[3], 1), 0, 1).astype(jnp.int32)
    return dict(targets=targets, partners=partners, pair_map=pair_map, shifts=shifts)


KPOINT_SCALING = 2.0
SCREENING_CUTOFF = 0.25
FORMS = ('anbm,pbxym->paxyn', 'anbm,pbxmz->paxnz', 'anbm,pbmyz->panyz')

def dft_tables(length):
    counter = jnp.arange(length, dtype=jnp.int32)
    product = counter[:, None] * counter[None, :] % length
    angles = product.astype(jnp.float32) * (2.0 * jnp.pi / length)
    cos_table = jnp.cos(angles)
    sine_lookup_table = jnp.sin(angles)
    forward = jnp.stack([jnp.stack([cos_table, sine_lookup_table], 1), jnp.stack([-sine_lookup_table, cos_table], 1)], 0)
    inverse = jnp.stack([jnp.stack([cos_table, -sine_lookup_table], 1), jnp.stack([sine_lookup_table, cos_table], 1)], 0)
    return (forward.astype(jnp.bfloat16), inverse.astype(jnp.bfloat16))

def coulomb(offset, shift, length):
    counter = jnp.arange(length, dtype=jnp.int32)
    frequency = ((counter + length // 2) % length - length // 2).astype(jnp.float32)
    lattice = (offset // 16, offset // 4 % 4, offset % 4)
    components = [frequency + shift[axis_id].astype(jnp.float32) + lattice[axis_id].astype(jnp.float32) * 0.25 for axis_id in range(3)]
    squared_magnitude = (components[0] * components[0])[:, None, None] + (components[1] * components[1])[None, :, None] + (components[2] * components[2])[None, None, :]
    return KPOINT_SCALING / (squared_magnitude + SCREENING_CUTOFF)

def rounded(values):
    return lax.optimization_barrier(values.astype(jnp.bfloat16))

def transform(exchange_matrix, blocks, form):
    return jnp.einsum(form, exchange_matrix.astype(jnp.float32), blocks.astype(jnp.float32))

def band_field(target, partners, kernel, forward, inverse, length):
    cells = length ** 3
    part_re = partners[:, 0].astype(jnp.float32)
    part_im = partners[:, 1].astype(jnp.float32)
    targ_re = target[0].astype(jnp.float32)
    targ_im = target[1].astype(jnp.float32)
    density = jnp.stack([part_re * targ_re + part_im * targ_im, part_re * targ_im - part_im * targ_re], 1)
    blocks = rounded(density).reshape(-1, 2, length, length, length)
    blocks = rounded(transform(forward, blocks, FORMS[0]))
    blocks = rounded(transform(forward, blocks, FORMS[1]))
    spectrum = transform(forward, blocks, FORMS[2])
    blocks = rounded(spectrum * kernel)
    blocks = rounded(transform(inverse, blocks, FORMS[2]))
    blocks = rounded(transform(inverse, blocks, FORMS[1]))
    potential = transform(inverse, blocks, FORMS[0]).reshape(-1, 2, cells) * (1.0 / cells)
    pot_re = potential[:, 0]
    pot_im = potential[:, 1]
    return -jnp.stack([jnp.sum(part_re * pot_re - part_im * pot_im, 0), jnp.sum(part_re * pot_im + part_im * pot_re, 0)], 0)

def real_vectors(fields):
    real_part = fields[:, 0]
    imag_part = fields[:, 1]
    return jnp.concatenate([jnp.concatenate([real_part, imag_part], 1), jnp.concatenate([-imag_part, real_part], 1)], 0)

def projector_of(target_set, summed, cells):
    basis_set = real_vectors(target_set.astype(jnp.float32))
    images = real_vectors(summed)
    intersection = jnp.dot(basis_set, images.T, precision=lax.Precision.HIGHEST) * (1.0 / cells)
    exchange_matrix = -0.5 * (intersection + intersection.T)
    prefactor_value = jnp.linalg.cholesky(exchange_matrix)
    solved = lax.linalg.triangular_solve(prefactor_value, images, left_side=True, lower=True)
    return solved.reshape(images.shape[0], 2, summed.shape[2])

def reference(targets, partners, pair_map, shifts):
    length = GRID
    cells = length ** 3
    forward, inverse = dft_tables(length)

    def one_target(k_row):
        target_set = targets[k_row]

        def append_partner_orbital(summed, q_row):
            kernel = coulomb(pair_map[k_row, q_row], shifts[k_row, q_row], length)
            occupied_orbitals = partners[q_row]
            fields = lax.map(lambda orbital: band_field(orbital, occupied_orbitals, kernel, forward, inverse, length), target_set)
            return (summed + fields, None)
        summed, unused = lax.scan(append_partner_orbital, jnp.zeros(target_set.shape, jnp.float32), jnp.arange(NQ, dtype=jnp.int32))
        return projector_of(target_set, summed, cells)
    return lax.map(one_target, jnp.arange(NK, dtype=jnp.int32))
```

```python
import jax
import jax.numpy as jnp
import numpy as np
from jax import lax
from jax.experimental import pallas as pl
from jax.experimental.pallas import tpu as pltpu
from jax.sharding import PartitionSpec as P

GRID = 32
BANDS = 4
OCC = 2
PLANE = 8
ROWS = GRID * PLANE
CELLS = GRID**3
KPOINT_SCALING = 2.0
SCREENING_CUTOFF = 0.25
PAIRS = [(i, j) for i in range(BANDS) for j in range(i, BANDS)]
EXTRA = 8


def phases(angle):
    turn = 2.0 * np.pi * (angle % GRID) / GRID
    return np.cos(turn), np.sin(turn)


def tables():
    row = np.arange(ROWS)
    lane = np.arange(128)
    hi, lo = row // PLANE, row % PLANE
    cos, sin = phases(hi[:, None] * hi[None] + 4 * lo[:, None] * lo[None])
    left = np.block([[cos, sin], [-sin, cos]])
    part, z = lane // GRID, lane % GRID
    cos, sin = phases(z[:, None] * z[None] + 8 * part[:, None] * part[None])
    right = np.block([[cos, -sin], [sin, cos]])
    twist = np.stack(phases(lo[:, None] * part[None]))
    return left.astype(jnp.bfloat16), right.astype(jnp.bfloat16), twist.astype(np.float32)


def wave_number(index):
    return ((index + GRID // 2) % GRID - GRID // 2).astype(jnp.float32)


def coulomb(offset, shift):
    row = lax.broadcasted_iota(jnp.int32, (ROWS, 128), 0)
    lane = lax.broadcasted_iota(jnp.int32, (ROWS, 128), 1)
    index = (row // PLANE, (lane // GRID) * PLANE + row % PLANE, lane % GRID)
    lattice = (offset // 16, offset // 4 % 4, offset % 4)
    squared = jnp.zeros((ROWS, 128), jnp.float32)
    for axis in range(3):
        moved = shift[axis].astype(jnp.float32) + lattice[axis].astype(jnp.float32) * 0.25
        component = wave_number(index[axis]) + moved
        squared += component * component
    return KPOINT_SCALING / (squared + SCREENING_CUTOFF)


def product(a, b):
    return jnp.dot(a, b, preferred_element_type=jnp.float32)


def exchange_kernel(offset, shift, targets, partners, left, right, twist, out, kernel):
    kernel[...] = coulomb(offset[0, 0], [shift[0, 0, axis] for axis in range(3)]) * (1.0 / CELLS)
    part_re = [partners[:, 16 * j : 16 * j + 8].astype(jnp.float32).reshape(ROWS, 128) for j in range(OCC)]
    part_im = [partners[:, 16 * j + 8 : 16 * j + 16].astype(jnp.float32).reshape(ROWS, 128) for j in range(OCC)]

    def twisted(re, im):
        return re * twist[0] + im * twist[1], im * twist[0] - re * twist[1]

    sums = {}
    for i in range(BANDS):
        targ_re = targets[2 * i].astype(jnp.float32)
        targ_im = targets[2 * i + 1].astype(jnp.float32)
        top = jnp.concatenate([part_re[j] * targ_re + part_im[j] * targ_im for j in range(OCC)], 1)
        bottom = jnp.concatenate([part_re[j] * targ_im - part_im[j] * targ_re for j in range(OCC)], 1)
        blocks = product(left[...], jnp.concatenate([top, bottom], 0).astype(jnp.bfloat16))
        rows = []
        for j in range(OCC):
            cut = slice(128 * j, 128 * j + 128)
            pair = twisted(blocks[:ROWS, cut], blocks[ROWS:, cut])
            rows.append(jnp.concatenate(pair, 1).astype(jnp.bfloat16))
        tops, bottoms = [], []
        for j in range(OCC):
            spectrum = product(rows[j], right[...])
            scaled = jnp.concatenate([spectrum[:, :128] * kernel[...], spectrum[:, 128:] * -kernel[...]], 1)
            back = product(scaled.astype(jnp.bfloat16), right[...])
            re, im = twisted(back[:, :128], back[:, 128:])
            tops.append(re)
            bottoms.append(im)
        stacked = jnp.concatenate([jnp.concatenate(tops, 1), jnp.concatenate(bottoms, 1)], 0)
        conjugate = product(left[...], stacked.astype(jnp.bfloat16))
        field_re = jnp.zeros((ROWS, 128), jnp.float32)
        field_im = jnp.zeros((ROWS, 128), jnp.float32)
        for j in range(OCC):
            cut = slice(128 * j, 128 * j + 128)
            re, im = conjugate[:ROWS, cut], conjugate[ROWS:, cut]
            field_re -= part_re[j] * re + part_im[j] * im
            field_im += part_re[j] * im - part_im[j] * re
        out[:, 32 * i : 32 * i + 16] = field_re.astype(jnp.bfloat16).reshape(16, 16, 128)
        out[:, 32 * i + 16 : 32 * i + 32] = field_im.astype(jnp.bfloat16).reshape(16, 16, 128)
        for other in range(i + 1):
            base_re = targets[2 * other].astype(jnp.float32)
            base_im = targets[2 * other + 1].astype(jnp.float32)
            same = base_re * field_re + base_im * field_im
            sums[other, i, 0] = same.reshape(GRID, 8, 128).sum(0)
            if other < i:
                cross = base_im * field_re - base_re * field_im
                sums[other, i, 1] = cross.reshape(GRID, 8, 128).sum(0)
    keys = [(i, j, 0) for i, j in PAIRS] + [(i, j, 1) for i, j in PAIRS if i < j]
    totals = jnp.concatenate([jnp.sum(sums[key], 0, keepdims=True) for key in keys], 0)
    totals = jnp.broadcast_to(jnp.sum(totals, 1, keepdims=True), (16, 128))
    lane = lax.broadcasted_iota(jnp.int32, (8, 128), 1)
    value = jnp.where(lane < 64, totals[:8], totals[8:])
    high = value.astype(jnp.bfloat16).astype(jnp.float32)
    middle = (value - high).astype(jnp.bfloat16).astype(jnp.float32)
    low = value - high - middle
    piece = lane % 64 // 16
    value = jnp.where(piece == 0, high, jnp.where(piece == 1, middle, jnp.where(piece == 2, low, 0.0)))
    out[:, 32 * BANDS :] = jnp.broadcast_to(value.astype(jnp.bfloat16)[None], (16, EXTRA, 128))


def exchange(offset, shift, targets, partners):
    left, right, twist = (jnp.asarray(table) for table in tables())
    smem = pl.BlockSpec(memory_space=pltpu.SMEM)
    vmem = pl.BlockSpec(memory_space=pltpu.VMEM)
    return pl.pallas_call(
        exchange_kernel,
        out_shape=jax.ShapeDtypeStruct((16, 32 * BANDS + EXTRA, 128), jnp.bfloat16),
        in_specs=[smem, smem, vmem, vmem, vmem, vmem, vmem],
        out_specs=vmem,
        scratch_shapes=[pltpu.VMEM((ROWS, 128), jnp.float32)],
        compiler_params=pltpu.CompilerParams(vmem_limit_bytes=24 << 20),
        name="exchange",
    )(offset, shift, targets, partners, left, right, twist)


def projector_kernel(shares, out):
    total = shares[0].astype(jnp.float32)
    for source in range(1, 16):
        total += shares[source].astype(jnp.float32)
    values = total[32 * BANDS :]
    values = values + pltpu.roll(values, 112, 1) + pltpu.roll(values, 96, 1)
    values = values * (-1.0 / CELLS)
    count = len(PAIRS)
    keys = [(i, j, 0) for i, j in PAIRS] + [(i, j, 1) for i, j in PAIRS if i < j]
    value = {}
    for at, key in enumerate(keys):
        lane = 64 * (at // 8)
        value[key] = jnp.broadcast_to(values[at % 8 : at % 8 + 1, lane : lane + 1], (8, 128))

    def entry(row, column):
        i, j = row % BANDS, column % BANDS
        if row // BANDS == column // BANDS:
            return value[min(i, j), max(i, j), 0]
        if i == j:
            return None
        return -value[i, j, 1] if i < j else value[j, i, 1]

    size = 2 * BANDS
    factor, inverse = {}, {}
    for column in range(size):
        for row in range(column, size):
            rest = entry(row, column)
            for before in range(column):
                if (row, before) in factor and (column, before) in factor:
                    part = factor[row, before] * factor[column, before]
                    rest = -part if rest is None else rest - part
            if row == column:
                guess = lax.rsqrt(rest)
                inverse[row] = guess * (1.5 - 0.5 * rest * guess * guess)
            elif rest is not None:
                factor[row, column] = rest * inverse[column]
    solved = []
    for row in range(size):
        for_parts = []
        for part in range(2):
            at = 32 * (row % BANDS) + 16 * (part if row < BANDS else 1 - part)
            rest = total[at : at + 16].reshape(2, 8, 128)
            if row >= BANDS and part == 0:
                rest = -rest
            for before in range(row):
                if (row, before) in factor:
                    rest = rest - factor[row, before][None] * solved[before][part]
            rest = rest * inverse[row][None]
            for_parts.append(rest)
            out[pl.ds(32 * row + part, 16, 2), :] = rest.reshape(16, 128)
        solved.append(for_parts)


def projector(shares):
    vmem = pl.BlockSpec(memory_space=pltpu.VMEM)
    return pl.pallas_call(
        projector_kernel,
        out_shape=jax.ShapeDtypeStruct((256, 128), jnp.float32),
        in_specs=[vmem],
        out_specs=vmem,
        compiler_params=pltpu.CompilerParams(vmem_limit_bytes=4 << 20),
        name="projector",
    )(shares)


def local(targets, partners, pair_map, shifts):
    plane = partners.reshape(1, 4 * PLANE, 128)
    gathered = lax.all_to_all(
        jnp.broadcast_to(plane, (GRID, 4 * PLANE, 128)), "ka", 0, 0, tiled=True
    )
    shares = exchange(pair_map, shifts, targets.reshape(2 * BANDS, ROWS, 128), gathered)
    shares = lax.all_to_all(shares, "pb", 0, 0, tiled=True)
    rows = projector(shares).reshape(2 * BANDS, 16, 2, 128)
    return jnp.swapaxes(rows, 1, 2).reshape(1, 2 * BANDS, 2, 2048)


def solution(mesh):
    return jax.shard_map(
        local,
        mesh=mesh,
        in_specs=(
            P("ka", None, None, None),
            P("pb", None, None, "ka"),
            P("ka", "pb"),
            P("ka", "pb", None),
        ),
        out_specs=P("ka", None, None, "pb"),
        check_vma=False,
    )
```

```python
import jax
import jax.numpy as jnp
import numpy as np
from jax import lax
from jax.experimental import pallas as pl
from jax.experimental.pallas import tpu as pltpu
from jax.sharding import Mesh
from jax.sharding import PartitionSpec as P

GRID = 32
BANDS = 4
OWN = 2
PLANE = 8
ROWS = GRID * PLANE
CELLS = GRID**3
KPOINT_SCALING = 2.0
SCREENING_CUTOFF = 0.25
FIELD_ROWS = 32 * OWN
EXTRA = 8


def phases(angle):
    turn = 2.0 * np.pi * (angle % GRID) / GRID
    return np.cos(turn), np.sin(turn)


def tables():
    row = np.arange(ROWS)
    lane = np.arange(128)
    hi, lo = row // PLANE, row % PLANE
    cos, sin = phases(hi[:, None] * hi[None] + 4 * lo[:, None] * lo[None])
    left = np.block([[cos, sin], [-sin, cos]])
    part, z = lane // GRID, lane % GRID
    cos, sin = phases(z[:, None] * z[None] + 8 * part[:, None] * part[None])
    right = np.block([[cos, -sin], [sin, cos]])
    twist = np.stack(phases(lo[:, None] * part[None]))
    return left.astype(jnp.bfloat16), right.astype(jnp.bfloat16), twist.astype(np.float32)


def wave_number(index):
    return ((index + GRID // 2) % GRID - GRID // 2).astype(jnp.float32)


def coulomb(offset, shift):
    row = lax.broadcasted_iota(jnp.int32, (ROWS, 128), 0)
    lane = lax.broadcasted_iota(jnp.int32, (ROWS, 128), 1)
    index = (row // PLANE, (lane // GRID) * PLANE + row % PLANE, lane % GRID)
    lattice = (offset // 16, offset // 4 % 4, offset % 4)
    squared = jnp.zeros((ROWS, 128), jnp.float32)
    for axis in range(3):
        moved = shift[axis].astype(jnp.float32) + lattice[axis].astype(jnp.float32) * 0.25
        component = wave_number(index[axis]) + moved
        squared += component * component
    return KPOINT_SCALING / (squared + SCREENING_CUTOFF)


def product(a, b):
    return jnp.dot(a, b, preferred_element_type=jnp.float32)


def spread_kernel(plane, out):
    out[...] = jnp.broadcast_to(plane[...][None], out.shape)


def prepare_kernel(mine, theirs, targets, kernel, parts, rows):
    place = mine[0, 4]
    for q in range(2):
        number = [jnp.where(place == q, mine[0, at], theirs[0, at]) for at in range(4)]
        kernel[q] = coulomb(number[0], number[1:]) * (1.0 / CELLS)
    for slot in range(BANDS):
        rows[...] = targets[(2 * place + slot) % BANDS].astype(jnp.float32)
        for part in range(2):
            parts[slot, part] = rows[pl.ds(part, ROWS, 2), :]


def fields_of(kernel, targets, gathered, left, right, twist, rows, parts):
    rows[...] = gathered[...].astype(jnp.float32).reshape(4 * ROWS, 128)
    for q in range(2):
        for part in range(2):
            parts[q, part] = rows[pl.ds(2 * ROWS * q + part, ROWS, 2), :]

    def twisted(re, im):
        return re * twist[0] + im * twist[1], im * twist[0] - re * twist[1]

    for band in range(OWN):
        tops, bottoms = [], []
        for q in range(2):
            tops.append(parts[q, 0] * targets[band, 0] + parts[q, 1] * targets[band, 1])
            bottoms.append(parts[q, 0] * targets[band, 1] - parts[q, 1] * targets[band, 0])
        density = jnp.concatenate([jnp.concatenate(tops, 1), jnp.concatenate(bottoms, 1)], 0)
        blocks = product(left[...], density.astype(jnp.bfloat16))
        tops, bottoms = [], []
        for q in range(2):
            cut = slice(128 * q, 128 * q + 128)
            pair = twisted(blocks[:ROWS, cut], blocks[ROWS:, cut])
            spectrum = product(jnp.concatenate(pair, 1).astype(jnp.bfloat16), right[...])
            scaled = jnp.concatenate(
                [spectrum[:, :128] * kernel[q], spectrum[:, 128:] * -kernel[q]], 1
            )
            back = product(scaled.astype(jnp.bfloat16), right[...])
            re, im = twisted(back[:, :128], back[:, 128:])
            tops.append(re)
            bottoms.append(im)
        stacked = jnp.concatenate([jnp.concatenate(tops, 1), jnp.concatenate(bottoms, 1)], 0)
        conjugate = product(left[...], stacked.astype(jnp.bfloat16))
        re_sum, im_sum = None, None
        for q in range(2):
            cut = slice(128 * q, 128 * q + 128)
            re, im = conjugate[:ROWS, cut], conjugate[ROWS:, cut]
            re_now = -(parts[q, 0] * re) - parts[q, 1] * im
            im_now = parts[q, 0] * im - parts[q, 1] * re
            re_sum = re_now if re_sum is None else re_sum + re_now
            im_sum = im_now if im_sum is None else im_sum + im_now
        yield band, re_sum, im_sum


def first_kernel(kernel, targets, gathered, left, right, twist, out, rows, parts):
    for band, re, im in fields_of(kernel, targets, gathered, left, right, twist, rows, parts):
        out[band, 0] = re
        out[band, 1] = im


def second_kernel(kernel, targets, gathered, left, right, twist, before, out, rows, parts):
    same, cross = {}, {}
    for band, re, im in fields_of(kernel, targets, gathered, left, right, twist, rows, parts):
        re += before[band, 0]
        im += before[band, 1]
        out[:, 32 * band : 32 * band + 16] = re.astype(jnp.bfloat16).reshape(16, 16, 128)
        out[:, 32 * band + 16 : 32 * band + 32] = im.astype(jnp.bfloat16).reshape(16, 16, 128)
        for slot in range(BANDS):
            total = targets[slot, 0] * re + targets[slot, 1] * im
            same[slot, band] = total.reshape(GRID, 8, 128).sum(0)
            total = targets[slot, 1] * re - targets[slot, 0] * im
            cross[slot, band] = total.reshape(GRID, 8, 128).sum(0)
    keys = [(slot, band) for slot in range(BANDS) for band in range(OWN)]
    totals = [jnp.sum(group[key], 0, keepdims=True) for group in (same, cross) for key in keys]
    totals = jnp.sum(jnp.concatenate(totals, 0), 1, keepdims=True)
    totals = jnp.broadcast_to(totals, (16, 128))
    lane = lax.broadcasted_iota(jnp.int32, (8, 128), 1)
    value = jnp.where(lane < 64, totals[:8], totals[8:])
    high = value.astype(jnp.bfloat16).astype(jnp.float32)
    middle = (value - high).astype(jnp.bfloat16).astype(jnp.float32)
    low = value - high - middle
    piece = lane % 64 // 16
    value = jnp.where(piece == 0, high, jnp.where(piece == 1, middle, jnp.where(piece == 2, low, 0.0)))
    out[:, FIELD_ROWS:] = jnp.broadcast_to(value.astype(jnp.bfloat16)[None], (16, EXTRA, 128))


def projector_kernel(shares, out):
    totals = []
    for group in range(2):
        total = shares[8 * group].astype(jnp.float32)
        for source in range(8 * group + 1, 8 * group + 8):
            total += shares[source].astype(jnp.float32)
        totals.append(total)
    same, cross = {}, {}
    for group in range(2):
        values = totals[group][FIELD_ROWS:]
        values = values + pltpu.roll(values, 112, 1) + pltpu.roll(values, 96, 1)
        values = values * (1.0 / CELLS)
        for slot in range(BANDS):
            for band in range(OWN):
                at = OWN * slot + band
                key = (2 * group + slot) % BANDS, 2 * group + band
                same[key] = jnp.broadcast_to(values[at : at + 1, 0:1], (8, 128))
                cross[key] = jnp.broadcast_to(values[at : at + 1, 64:65], (8, 128))

    def entry(row, column):
        i, j = row % BANDS, column % BANDS
        if row // BANDS == column // BANDS:
            return -0.5 * (same[i, j] + same[j, i])
        return None if i == j else 0.5 * (cross[i, j] - cross[j, i])

    size = 2 * BANDS
    factor, inverse = {}, {}
    for column in range(size):
        for row in range(column, size):
            rest = entry(row, column)
            for before in range(column):
                if (row, before) in factor and (column, before) in factor:
                    part = factor[row, before] * factor[column, before]
                    rest = -part if rest is None else rest - part
            if row == column:
                guess = lax.rsqrt(rest)
                inverse[row] = guess * (1.5 - 0.5 * rest * guess * guess)
            elif rest is not None:
                factor[row, column] = rest * inverse[column]
    solved = []
    for row in range(size):
        for_parts = []
        for part in range(2):
            band = row % BANDS
            at = 32 * (band % OWN) + 16 * (part if row < BANDS else 1 - part)
            rest = totals[band // OWN][at : at + 16].reshape(2, 8, 128)
            if row >= BANDS and part == 0:
                rest = -rest
            for before in range(row):
                if (row, before) in factor:
                    rest = rest - factor[row, before][None] * solved[before][part]
            rest = rest * inverse[row][None]
            for_parts.append(rest)
            out[pl.ds(32 * row + part, 16, 2), :] = rest.reshape(16, 128)
        solved.append(for_parts)


SMEM = pl.BlockSpec(memory_space=pltpu.SMEM)
VMEM = pl.BlockSpec(memory_space=pltpu.VMEM)


def call(kernel, name, shapes, specs, scratch, limit, *operands):
    return pl.pallas_call(
        kernel,
        out_shape=shapes,
        in_specs=specs,
        out_specs=jax.tree.map(lambda _: VMEM, shapes),
        scratch_shapes=scratch,
        compiler_params=pltpu.CompilerParams(vmem_limit_bytes=limit << 20),
        name=name,
    )(*operands)


def array(*shape, dtype=jnp.float32):
    return jax.ShapeDtypeStruct(shape, dtype)


def spread(plane):
    shape = array(GRID, 4 * PLANE, 128, dtype=jnp.bfloat16)
    return call(spread_kernel, "spread", shape, [VMEM], [], 1, plane)


def prepare(mine, theirs, targets):
    shapes = (array(2, ROWS, 128), array(BANDS, 2, ROWS, 128))
    scratch = [pltpu.VMEM((2 * ROWS, 128), jnp.float32)]
    return call(prepare_kernel, "prepare", shapes, [SMEM, SMEM, VMEM], scratch, 8, mine, theirs, targets)


def exchange(*operands):
    scratch = [pltpu.VMEM((4 * ROWS, 128), jnp.float32), pltpu.VMEM((2, 2, ROWS, 128), jnp.float32)]
    specs = [VMEM] * len(operands)
    if len(operands) == 6:
        return call(first_kernel, "first", array(OWN, 2, ROWS, 128), specs, scratch, 16, *operands)
    shape = array(16, FIELD_ROWS + EXTRA, 128, dtype=jnp.bfloat16)
    return call(second_kernel, "second", shape, specs, scratch, 16, *operands)


def projector(shares):
    return call(projector_kernel, "projector", array(256, 128), [VMEM], [], 4, shares)


def interleaved(values):
    tiles = values.reshape(values.shape[0], 2, values.shape[2] // 128, 128)
    return jnp.swapaxes(tiles, 1, 2).reshape(values.shape[0], -1, 128)


def local(targets, partners, pair_map, shifts):
    left, right, twist = (jnp.asarray(table) for table in tables())
    place = lax.axis_index("xh")
    operand = spread(interleaved(partners[0]).reshape(4 * PLANE, 128)).reshape(2 * GRID, 2 * PLANE, 128)
    gathered = lax.all_to_all(operand, ("xh", "ka"), 0, 0, tiled=True)
    mine = jnp.concatenate([pair_map, shifts[0], place.reshape(1, 1)], 1)
    theirs = lax.ppermute(mine, "xh", [(0, 1), (1, 0)])
    kernel, parts = prepare(mine, theirs, interleaved(targets[0]))
    gathered, kernel, parts = lax.optimization_barrier((gathered, kernel, parts))
    count = lax.axis_size("ka")
    swapped = lax.ppermute(gathered, "ka", [(i, i ^ 1) for i in range(count)])
    before = exchange(kernel, parts, gathered, left, right, twist)
    shares = exchange(kernel, parts, swapped, left, right, twist, before)
    shares = lax.all_to_all(shares, ("xh", "zz"), 0, 0, tiled=True)
    rows = projector(shares).reshape(2 * BANDS, 16, 2, 128)
    return jnp.swapaxes(rows, 1, 2).reshape(1, 2 * BANDS, 2, 2048)


def solution(mesh):
    split = Mesh(mesh.devices.reshape(GRID, 2, 8), ("ka", "xh", "zz"))
    return jax.shard_map(
        local,
        mesh=split,
        in_specs=(
            P("ka", None, None, None),
            P(("xh", "zz"), None, None, "ka"),
            P("ka", ("xh", "zz")),
            P("ka", ("xh", "zz"), None),
        ),
        out_specs=P("ka", None, None, ("xh", "zz")),
        check_vma=False,
    )
```

```python
import jax
import jax.numpy as jnp
import numpy as np
from jax import lax
from jax.experimental import pallas as pl
from jax.experimental.pallas import tpu as pltpu
from jax.sharding import Mesh
from jax.sharding import PartitionSpec as P

GRID = 32
BANDS = 4
OWN = 2
PLANE = 8
ROWS = GRID * PLANE
CELLS = GRID**3
KPOINT_SCALING = 2.0
SCREENING_CUTOFF = 0.25
FIELD_ROWS = 32 * OWN
EXTRA = 8
PAIRS = [(0, 0, 0), (1, 1, 0), (0, 1, 0), (0, 1, 1), (2, 0, 0), (2, 0, 1), (3, 1, 0), (3, 1, 1)]


def phases(angle):
    turn = 2.0 * np.pi * (angle % GRID) / GRID
    return np.cos(turn), np.sin(turn)


def tables():
    row = np.arange(ROWS)
    lane = np.arange(128)
    hi, lo = row // PLANE, row % PLANE
    cos, sin = phases(hi[:, None] * hi[None] + 4 * lo[:, None] * lo[None])
    left = np.block([[cos, sin], [-sin, cos]])
    part, z = lane // GRID, lane % GRID
    cos, sin = phases(z[:, None] * z[None] + 8 * part[:, None] * part[None])
    right = np.block([[cos, -sin], [sin, cos]])
    twist = np.stack(phases(lo[:, None] * part[None]))
    return left.astype(jnp.bfloat16), right.astype(jnp.bfloat16), twist.astype(np.float32)


def wave_number(index):
    return ((index + GRID // 2) % GRID - GRID // 2).astype(jnp.float32)


def coulomb(offset, shift):
    row = lax.broadcasted_iota(jnp.int32, (ROWS, 128), 0)
    lane = lax.broadcasted_iota(jnp.int32, (ROWS, 128), 1)
    index = (row // PLANE, (lane // GRID) * PLANE + row % PLANE, lane % GRID)
    lattice = (offset // 16, offset // 4 % 4, offset % 4)
    squared = jnp.zeros((ROWS, 128), jnp.float32)
    for axis in range(3):
        moved = shift[axis].astype(jnp.float32) + lattice[axis].astype(jnp.float32) * 0.25
        component = wave_number(index[axis]) + moved
        squared += component * component
    return KPOINT_SCALING / (squared + SCREENING_CUTOFF)


def product(a, b):
    return jnp.dot(a, b, preferred_element_type=jnp.float32)


def coulomb_kernel(mine, theirs, kernel):
    place = mine[0, 4]
    for q in range(2):
        number = [jnp.where(place == q, mine[0, at], theirs[0, at]) for at in range(4)]
        kernel[q] = coulomb(number[0], number[1:]) * (1.0 / CELLS)


def apart_kernel(place, targets, parts, rows):
    for slot in range(BANDS):
        rows[...] = targets[band_of(slot, place[0, 0])].astype(jnp.float32)
        for part in range(2):
            parts[slot, part] = rows[pl.ds(part, ROWS, 2), :]


def band_of(slot, place):
    return 2 * place + slot if slot < OWN else slot - (1 + 2 * (slot - OWN)) * place


def fields_of(kernel, targets, gathered, left, right, twist, rows, parts):
    rows[...] = gathered[...].astype(jnp.float32).reshape(4 * ROWS, 128)
    for q in range(2):
        for part in range(2):
            parts[q, part] = rows[pl.ds(2 * ROWS * q + part, ROWS, 2), :]

    def twisted(re, im):
        return re * twist[0] + im * twist[1], im * twist[0] - re * twist[1]

    def density(band):
        tops, bottoms = [], []
        for q in range(2):
            tops.append(parts[q, 0] * targets[band, 0] + parts[q, 1] * targets[band, 1])
            bottoms.append(parts[q, 0] * targets[band, 1] - parts[q, 1] * targets[band, 0])
        return joined(tops, bottoms)

    def joined(tops, bottoms):
        rows = [jnp.concatenate(tops, 1), jnp.concatenate(bottoms, 1)]
        return jnp.concatenate(rows, 0).astype(jnp.bfloat16)

    def to_spectrum(blocks):
        pairs = []
        for q in range(2):
            cut = slice(128 * q, 128 * q + 128)
            pair = twisted(blocks[:ROWS, cut], blocks[ROWS:, cut])
            pairs.append(jnp.concatenate(pair, 1).astype(jnp.bfloat16))
        return product(jnp.concatenate(pairs, 0), right[...])

    def from_spectrum(spectrum):
        scaled = []
        for q in range(2):
            cut = slice(ROWS * q, ROWS * q + ROWS)
            pair = spectrum[cut, :128] * kernel[q], spectrum[cut, 128:] * -kernel[q]
            scaled.append(jnp.concatenate(pair, 1).astype(jnp.bfloat16))
        return product(jnp.concatenate(scaled, 0), right[...])

    def untwisted(back):
        tops, bottoms = [], []
        for q in range(2):
            cut = slice(ROWS * q, ROWS * q + ROWS)
            re, im = twisted(back[cut, :128], back[cut, 128:])
            tops.append(re)
            bottoms.append(im)
        return joined(tops, bottoms)

    def field(conjugate):
        re_sum, im_sum = None, None
        for q in range(2):
            cut = slice(128 * q, 128 * q + 128)
            re, im = conjugate[:ROWS, cut], conjugate[ROWS:, cut]
            re_now = -(parts[q, 0] * re) - parts[q, 1] * im
            im_now = parts[q, 0] * im - parts[q, 1] * re
            re_sum = re_now if re_sum is None else re_sum + re_now
            im_sum = im_now if im_sum is None else im_sum + im_now
        return re_sum, im_sum

    values = [product(left[...], density(band)) for band in range(OWN)]
    values = [to_spectrum(value) for value in values]
    values = [from_spectrum(value) for value in values]
    values = [product(left[...], untwisted(value)) for value in values]
    for band, value in enumerate(values):
        yield (band, *field(value))


def first_kernel(kernel, targets, gathered, left, right, twist, out, rows, parts):
    for band, re, im in fields_of(kernel, targets, gathered, left, right, twist, rows, parts):
        out[band, 0] = re
        out[band, 1] = im


def second_kernel(kernel, targets, gathered, left, right, twist, before, out, rows, parts):
    sums = {}
    for band, re, im in fields_of(kernel, targets, gathered, left, right, twist, rows, parts):
        re += before[band, 0]
        im += before[band, 1]
        out[:, 32 * band : 32 * band + 16] = re.astype(jnp.bfloat16).reshape(16, 16, 128)
        out[:, 32 * band + 16 : 32 * band + 32] = im.astype(jnp.bfloat16).reshape(16, 16, 128)
        for slot, own, cross in PAIRS:
            if own == band:
                if cross:
                    total = targets[slot, 1] * re - targets[slot, 0] * im
                else:
                    total = targets[slot, 0] * re + targets[slot, 1] * im
                sums[slot, own, cross] = total.reshape(GRID, 8, 128).sum(0)
    value = jnp.concatenate([jnp.sum(sums[key], 0, keepdims=True) for key in PAIRS], 0)
    value = jnp.broadcast_to(jnp.sum(value, 1, keepdims=True), (8, 128))
    piece = lax.broadcasted_iota(jnp.int32, (8, 128), 1) // 32
    high = value.astype(jnp.bfloat16).astype(jnp.float32)
    middle = (value - high).astype(jnp.bfloat16).astype(jnp.float32)
    low = value - high - middle
    value = jnp.where(piece == 0, high, jnp.where(piece == 1, middle, jnp.where(piece == 2, low, 0.0)))
    out[:, FIELD_ROWS:] = jnp.broadcast_to(value.astype(jnp.bfloat16)[None], (16, EXTRA, 128))


def projector_kernel(shares, out):
    totals = []
    for group in range(2):
        total = shares[8 * group].astype(jnp.float32)
        for source in range(8 * group + 1, 8 * group + 8):
            total += shares[source].astype(jnp.float32)
        totals.append(total)
    value = {}
    for group in range(2):
        values = totals[group][FIELD_ROWS:]
        values = values + pltpu.roll(values, 96, 1) + pltpu.roll(values, 64, 1)
        values = values * (1.0 / CELLS)
        for at, (slot, own, cross) in enumerate(PAIRS):
            key = band_of(slot, group), band_of(own, group), cross
            value[key] = jnp.broadcast_to(values[at : at + 1, 0:1], (8, 128))

    def entry(row, column):
        i, j = row % BANDS, column % BANDS
        if row // BANDS == column // BANDS:
            return -(value[i, j, 0] if (i, j, 0) in value else value[j, i, 0])
        if i == j:
            return None
        return value[i, j, 1] if (i, j, 1) in value else -value[j, i, 1]

    size = 2 * BANDS
    factor, inverse = {}, {}
    for column in range(size):
        for row in range(column, size):
            rest = entry(row, column)
            for before in range(column):
                if (row, before) in factor and (column, before) in factor:
                    part = factor[row, before] * factor[column, before]
                    rest = -part if rest is None else rest - part
            if row == column:
                guess = lax.rsqrt(rest)
                inverse[row] = guess * (1.5 - 0.5 * rest * guess * guess)
            elif rest is not None:
                factor[row, column] = rest * inverse[column]
    solved = []
    for row in range(size):
        for_parts = []
        for part in range(2):
            band = row % BANDS
            at = 32 * (band % OWN) + 16 * (part if row < BANDS else 1 - part)
            rest = totals[band // OWN][at : at + 16].reshape(2, 8, 128)
            if row >= BANDS and part == 0:
                rest = -rest
            for before in range(row):
                if (row, before) in factor:
                    rest = rest - factor[row, before][None] * solved[before][part]
            rest = rest * inverse[row][None]
            for_parts.append(rest)
            out[pl.ds(32 * row + part, 16, 2), :] = rest.reshape(16, 128)
        solved.append(for_parts)


SMEM = pl.BlockSpec(memory_space=pltpu.SMEM)
VMEM = pl.BlockSpec(memory_space=pltpu.VMEM)


def call(kernel, name, shapes, specs, scratch, limit, *operands):
    return pl.pallas_call(
        kernel,
        out_shape=shapes,
        in_specs=specs,
        out_specs=jax.tree.map(lambda _: VMEM, shapes),
        scratch_shapes=scratch,
        compiler_params=pltpu.CompilerParams(vmem_limit_bytes=limit << 20),
        name=name,
    )(*operands)


def array(*shape, dtype=jnp.float32):
    return jax.ShapeDtypeStruct(shape, dtype)


def prepare(mine, theirs):
    return call(coulomb_kernel, "coulomb", array(2, ROWS, 128), [SMEM, SMEM], [], 2, mine, theirs)


def apart(place, targets):
    scratch = [pltpu.VMEM((2 * ROWS, 128), jnp.float32)]
    shape = array(BANDS, 2, ROWS, 128)
    return call(apart_kernel, "apart", shape, [SMEM, VMEM], scratch, 4, place, targets)


def exchange(*operands):
    scratch = [pltpu.VMEM((4 * ROWS, 128), jnp.float32), pltpu.VMEM((2, 2, ROWS, 128), jnp.float32)]
    specs = [VMEM] * len(operands)
    if len(operands) == 6:
        return call(first_kernel, "first", array(OWN, 2, ROWS, 128), specs, scratch, 16, *operands)
    shape = array(16, FIELD_ROWS + EXTRA, 128, dtype=jnp.bfloat16)
    return call(second_kernel, "second", shape, specs, scratch, 16, *operands)


def projector(shares):
    return call(projector_kernel, "projector", array(256, 128), [VMEM], [], 4, shares)


def interleaved(values):
    tiles = values.reshape(values.shape[0], 2, values.shape[2] // 128, 128)
    return jnp.swapaxes(tiles, 1, 2).reshape(values.shape[0], -1, 128)


def local(targets, partners, pair_map, shifts):
    left, right, twist = (jnp.asarray(table) for table in tables())
    place = lax.axis_index("xh")
    plane = interleaved(partners[0]).reshape(1, 4 * PLANE, 128)
    operand = jnp.broadcast_to(plane, (GRID, 4 * PLANE, 128)).reshape(2 * GRID, 2 * PLANE, 128)
    gathered = lax.all_to_all(operand, ("xh", "ka"), 0, 0, tiled=True)
    mine = jnp.concatenate([pair_map, shifts[0], place.reshape(1, 1)], 1)
    theirs = lax.ppermute(mine, "xh", [(0, 1), (1, 0)])
    parts = apart(place.reshape(1, 1), interleaved(targets[0]))
    kernel = prepare(mine, theirs)
    gathered, kernel, parts = lax.optimization_barrier((gathered, kernel, parts))
    count = lax.axis_size("ka")
    swapped = lax.ppermute(gathered, "ka", [(i, i ^ 1) for i in range(count)])
    before = exchange(kernel, parts, gathered, left, right, twist)
    shares = exchange(kernel, parts, swapped, left, right, twist, before)
    shares = lax.all_to_all(shares, ("xh", "zz"), 0, 0, tiled=True)
    rows = projector(shares).reshape(2 * BANDS, 16, 2, 128)
    return jnp.swapaxes(rows, 1, 2).reshape(1, 2 * BANDS, 2, 2048)


def solution(mesh):
    split = Mesh(mesh.devices.reshape(GRID, 2, 8), ("ka", "xh", "zz"))
    return jax.shard_map(
        local,
        mesh=split,
        in_specs=(
            P("ka", None, None, None),
            P(("xh", "zz"), None, None, "ka"),
            P("ka", ("xh", "zz")),
            P("ka", ("xh", "zz"), None),
        ),
        out_specs=P("ka", None, None, ("xh", "zz")),
        check_vma=False,
    )
```

```python
import jax
import jax.numpy as jnp
import numpy as np
from jax import lax
from jax.experimental import pallas as pl
from jax.experimental.pallas import tpu as pltpu
from jax.sharding import Mesh
from jax.sharding import PartitionSpec as P

GRID = 32
BANDS = 4
OCC = 2
OWN = 2
PLANE = 8
ROWS = GRID * PLANE
CELLS = GRID**3
KPOINT_SCALING = 2.0
SCREENING_CUTOFF = 0.25
FIELD_ROWS = 32 * OWN
EXTRA = 8
PEERS = 32
NUMBERS = 8
PAIRS = [(0, 0, 0), (1, 1, 0), (0, 1, 0), (0, 1, 1), (2, 0, 0), (2, 0, 1), (3, 1, 0), (3, 1, 1)]


def phases(angle):
    turn = 2.0 * np.pi * (angle % GRID) / GRID
    return np.cos(turn), np.sin(turn)


def tables():
    row = np.arange(ROWS)
    lane = np.arange(128)
    hi, lo = row // PLANE, row % PLANE
    cos, sin = phases(hi[:, None] * hi[None] + 4 * lo[:, None] * lo[None])
    left = np.block([[cos, sin], [-sin, cos]])
    part, z = lane // GRID, lane % GRID
    cos, sin = phases(z[:, None] * z[None] + 8 * part[:, None] * part[None])
    right = np.block([[cos, -sin], [sin, cos]])
    twist = np.stack(phases(lo[:, None] * part[None]))
    return left.astype(jnp.bfloat16), right.astype(jnp.bfloat16), twist.astype(np.float32)


def wave_number(index):
    return ((index + GRID // 2) % GRID - GRID // 2).astype(jnp.float32)


def coulomb(offset, shift):
    row = lax.broadcasted_iota(jnp.int32, (ROWS, 128), 0)
    lane = lax.broadcasted_iota(jnp.int32, (ROWS, 128), 1)
    index = (row // PLANE, (lane // GRID) * PLANE + row % PLANE, lane % GRID)
    lattice = (offset // 16, offset // 4 % 4, offset % 4)
    squared = jnp.zeros((ROWS, 128), jnp.float32)
    for axis in range(3):
        moved = shift[axis].astype(jnp.float32) + lattice[axis].astype(jnp.float32) * 0.25
        component = wave_number(index[axis]) + moved
        squared += component * component
    return KPOINT_SCALING / (squared + SCREENING_CUTOFF)


def product(a, b):
    return jnp.dot(a, b, preferred_element_type=jnp.float32)


def spread_kernel(plane, offset, shift, out, tile, shift_now, arrive, leave):
    copies = [
        pltpu.make_async_copy(shift, shift_now, arrive.at[0]),
        pltpu.make_async_copy(plane, tile.at[0 : 4 * PLANE], arrive.at[1]),
    ]
    for copy in copies:
        copy.start()
    copies[0].wait()
    row = lax.broadcasted_iota(jnp.int32, (NUMBERS, 128), 0)
    value = jnp.zeros((NUMBERS, 128), jnp.int32) + offset[0, 0]
    for axis in range(3):
        value = jnp.where(row == axis + 1, shift_now[0, axis], value)
    tile[4 * PLANE :] = value.astype(jnp.float32).astype(jnp.bfloat16)
    copies[1].wait()
    copies = [pltpu.make_async_copy(tile, out.at[at], leave.at[at]) for at in range(PEERS)]
    for copy in copies:
        copy.start()
    for copy in copies:
        copy.wait()


def coulomb_kernel(place, gathered, kernel):
    for q in range(2):
        numbers = gathered[place[0, 0] + q * (PEERS // 2), 4 * PLANE :].astype(jnp.float32)
        numbers = numbers.astype(jnp.int32)
        shift = [numbers[axis + 1 : axis + 2] for axis in range(3)]
        kernel[q] = coulomb(numbers[0:1], shift) * (1.0 / CELLS)


def apart_kernel(place, targets, parts, rows):
    for slot in range(BANDS):
        rows[...] = targets[band_of(slot, place[0, 0])].astype(jnp.float32)
        for part in range(2):
            parts[slot, part] = rows[pl.ds(part, ROWS, 2), :]


def band_of(slot, place):
    return 2 * place + slot if slot < OWN else slot - (1 + 2 * (slot - OWN)) * place


def exchange_kernel(core, kernel, targets, own, other, left, right, twist, out, rows, parts):
    for source, parity in ((own, core[0, 0]), (other, 1 - core[0, 0])):
        for q in range(2):
            for j in range(OCC):
                planes = source[16 * q : 16 * q + 16, 16 * j : 16 * j + 16].astype(jnp.float32)
                rows[q, j, :, pl.ds(parity, 1)] = planes[:, None]
    for q in range(2):
        for j in range(OCC):
            for part in range(2):
                parts[j, q, part] = rows[q, j, :, :, pl.ds(part, PLANE, 2), :].reshape(ROWS, 128)

    def twisted(re, im):
        return re * twist[0] + im * twist[1], im * twist[0] - re * twist[1]

    def density(band, j):
        tops, bottoms = [], []
        for q in range(2):
            re, im = parts[j, q, 0], parts[j, q, 1]
            tops.append(re * targets[band, 0] + im * targets[band, 1])
            bottoms.append(re * targets[band, 1] - im * targets[band, 0])
        return joined(tops, bottoms)

    def joined(tops, bottoms):
        rows = [jnp.concatenate(tops, 1), jnp.concatenate(bottoms, 1)]
        return jnp.concatenate(rows, 0).astype(jnp.bfloat16)

    def to_spectrum(blocks):
        pairs = []
        for q in range(2):
            cut = slice(128 * q, 128 * q + 128)
            pair = twisted(blocks[:ROWS, cut], blocks[ROWS:, cut])
            pairs.append(jnp.concatenate(pair, 1).astype(jnp.bfloat16))
        return product(jnp.concatenate(pairs, 0), right[...])

    def from_spectrum(spectrum):
        scaled = []
        for q in range(2):
            cut = slice(ROWS * q, ROWS * q + ROWS)
            pair = spectrum[cut, :128] * kernel[q], spectrum[cut, 128:] * -kernel[q]
            scaled.append(jnp.concatenate(pair, 1).astype(jnp.bfloat16))
        return product(jnp.concatenate(scaled, 0), right[...])

    def untwisted(back):
        tops, bottoms = [], []
        for q in range(2):
            cut = slice(ROWS * q, ROWS * q + ROWS)
            re, im = twisted(back[cut, :128], back[cut, 128:])
            tops.append(re)
            bottoms.append(im)
        return joined(tops, bottoms)

    def field(conjugates):
        re_sum, im_sum = None, None
        for j in range(OCC):
            for q in range(2):
                cut = slice(128 * q, 128 * q + 128)
                re, im = conjugates[j][:ROWS, cut], conjugates[j][ROWS:, cut]
                re_now = -(parts[j, q, 0] * re) - parts[j, q, 1] * im
                im_now = parts[j, q, 0] * im - parts[j, q, 1] * re
                re_sum = re_now if re_sum is None else re_sum + re_now
                im_sum = im_now if im_sum is None else im_sum + im_now
        return re_sum, im_sum

    units = [(band, j) for band in range(OWN) for j in range(OCC)]
    values = [product(left[...], density(*unit)) for unit in units]
    values = [to_spectrum(value) for value in values]
    values = [from_spectrum(value) for value in values]
    values = [product(left[...], untwisted(value)) for value in values]
    sums = {}
    for band in range(OWN):
        re, im = field(values[OCC * band : OCC * band + OCC])
        out[:, 32 * band : 32 * band + 16] = re.astype(jnp.bfloat16).reshape(16, 16, 128)
        out[:, 32 * band + 16 : 32 * band + 32] = im.astype(jnp.bfloat16).reshape(16, 16, 128)
        for slot, place, cross in PAIRS:
            if place == band:
                if cross:
                    total = targets[slot, 1] * re - targets[slot, 0] * im
                else:
                    total = targets[slot, 0] * re + targets[slot, 1] * im
                sums[slot, place, cross] = total.reshape(GRID, 8, 128).sum(0)
    value = jnp.concatenate([jnp.sum(sums[key], 0, keepdims=True) for key in PAIRS], 0)
    value = jnp.broadcast_to(jnp.sum(value, 1, keepdims=True), (8, 128))
    piece = lax.broadcasted_iota(jnp.int32, (8, 128), 1) // 32
    high = value.astype(jnp.bfloat16).astype(jnp.float32)
    middle = (value - high).astype(jnp.bfloat16).astype(jnp.float32)
    low = value - high - middle
    value = jnp.where(piece == 0, high, jnp.where(piece == 1, middle, jnp.where(piece == 2, low, 0.0)))
    out[:, FIELD_ROWS:] = jnp.broadcast_to(value.astype(jnp.bfloat16)[None], (16, EXTRA, 128))


def projector_kernel(shares, out):
    totals = []
    for group in range(2):
        total = shares[8 * group].astype(jnp.float32)
        for source in range(8 * group + 1, 8 * group + 8):
            total += shares[source].astype(jnp.float32)
        totals.append(total)
    value = {}
    for group in range(2):
        values = totals[group][FIELD_ROWS:]
        values = values + pltpu.roll(values, 96, 1) + pltpu.roll(values, 64, 1)
        values = values * (1.0 / CELLS)
        for at, (slot, own, cross) in enumerate(PAIRS):
            key = band_of(slot, group), band_of(own, group), cross
            value[key] = jnp.broadcast_to(values[at : at + 1, 0:1], (8, 128))

    def entry(row, column):
        i, j = row % BANDS, column % BANDS
        if row // BANDS == column // BANDS:
            return -(value[i, j, 0] if (i, j, 0) in value else value[j, i, 0])
        if i == j:
            return None
        return value[i, j, 1] if (i, j, 1) in value else -value[j, i, 1]

    size = 2 * BANDS
    factor, inverse = {}, {}
    for column in range(size):
        for row in range(column, size):
            rest = entry(row, column)
            for before in range(column):
                if (row, before) in factor and (column, before) in factor:
                    part = factor[row, before] * factor[column, before]
                    rest = -part if rest is None else rest - part
            if row == column:
                guess = lax.rsqrt(rest)
                inverse[row] = guess * (1.5 - 0.5 * rest * guess * guess)
            elif rest is not None:
                factor[row, column] = rest * inverse[column]
    solved = []
    for row in range(size):
        for_parts = []
        for part in range(2):
            band = row % BANDS
            at = 32 * (band % OWN) + 16 * (part if row < BANDS else 1 - part)
            rest = totals[band // OWN][at : at + 16].reshape(2, 8, 128)
            if row >= BANDS and part == 0:
                rest = -rest
            for before in range(row):
                if (row, before) in factor:
                    rest = rest - factor[row, before][None] * solved[before][part]
            rest = rest * inverse[row][None]
            for_parts.append(rest)
            out[pl.ds(32 * row + part, 16, 2), :] = rest.reshape(16, 128)
        solved.append(for_parts)


SMEM = pl.BlockSpec(memory_space=pltpu.SMEM)
VMEM = pl.BlockSpec(memory_space=pltpu.VMEM)


def call(kernel, name, shapes, specs, scratch, limit, *operands):
    return pl.pallas_call(
        kernel,
        out_shape=shapes,
        in_specs=specs,
        out_specs=jax.tree.map(lambda _: VMEM, shapes),
        scratch_shapes=scratch,
        compiler_params=pltpu.CompilerParams(vmem_limit_bytes=limit << 20),
        name=name,
    )(*operands)


def array(*shape, dtype=jnp.float32):
    return jax.ShapeDtypeStruct(shape, dtype)


def stay(operand):
    return pltpu.with_memory_space_constraint(operand, pltpu.HBM)


def spread(plane, offset, shift):
    rows = 4 * PLANE + NUMBERS
    scratch = [
        pltpu.VMEM((rows, 128), jnp.bfloat16),
        pltpu.SMEM((1, 3), jnp.int32),
        pltpu.SemaphoreType.DMA((2,)),
        pltpu.SemaphoreType.DMA((PEERS,)),
    ]
    hbm = pl.BlockSpec(memory_space=pltpu.HBM)
    return pl.pallas_call(
        spread_kernel,
        out_shape=array(PEERS, rows, 128, dtype=jnp.bfloat16),
        in_specs=[hbm, SMEM, hbm],
        out_specs=hbm,
        scratch_shapes=scratch,
        compiler_params=pltpu.CompilerParams(vmem_limit_bytes=1 << 20),
        name="spread",
    )(stay(plane), offset, stay(shift))


def prepare(place, gathered):
    return call(coulomb_kernel, "coulomb", array(2, ROWS, 128), [SMEM, VMEM], [], 2, place, gathered)


def apart(place, targets):
    scratch = [pltpu.VMEM((2 * ROWS, 128), jnp.float32)]
    shape = array(BANDS, 2, ROWS, 128)
    return call(apart_kernel, "apart", shape, [SMEM, VMEM], scratch, 4, place, targets)


def exchange(*operands):
    scratch = [
        pltpu.VMEM((2, OCC, GRID // 2, 2, 2 * PLANE, 128), jnp.float32),
        pltpu.VMEM((OCC, 2, 2, ROWS, 128), jnp.float32),
    ]
    shape = array(16, FIELD_ROWS + EXTRA, 128, dtype=jnp.bfloat16)
    specs = [SMEM] + [VMEM] * (len(operands) - 1)
    return call(exchange_kernel, "exchange", shape, specs, scratch, 24, *operands)


def projector(shares):
    return call(projector_kernel, "projector", array(256, 128), [VMEM], [], 4, shares)


def interleaved(values):
    tiles = values.reshape(values.shape[0], 2, values.shape[2] // 128, 128)
    return jnp.swapaxes(tiles, 1, 2).reshape(values.shape[0], -1, 128)


def local(targets, partners, pair_map, shifts):
    left, right, twist = (jnp.asarray(table) for table in tables())
    place, core, group = (lax.axis_index(axis).reshape(1, 1) for axis in ("chip", "core", "xh"))
    plane = interleaved(partners[0]).reshape(4 * PLANE, 128)
    operand = spread(plane, pair_map, shifts[0])
    gathered = lax.all_to_all(operand, ("xh", "chip"), 0, 0, tiled=True)
    parts = apart(group, interleaved(targets[0]))
    gathered, parts = lax.optimization_barrier((gathered, parts))
    swapped = lax.ppermute(gathered, "core", [(0, 1), (1, 0)])
    kernel = prepare(place, gathered)
    shares = exchange(core, kernel, parts, gathered, swapped, left, right, twist)
    shares = lax.all_to_all(shares, ("xh", "zz"), 0, 0, tiled=True)
    rows = projector(shares).reshape(2 * BANDS, 16, 2, 128)
    return jnp.swapaxes(rows, 1, 2).reshape(1, 2 * BANDS, 2, 2048)


def solution(mesh):
    split = Mesh(mesh.devices.reshape(16, 2, 2, 8), ("chip", "core", "xh", "zz"))
    ka, pb = ("chip", "core"), ("xh", "zz")
    return jax.shard_map(
        local,
        mesh=split,
        in_specs=(
            P(ka, None, None, None),
            P(pb, None, None, ka),
            P(ka, pb),
            P(ka, pb, None),
        ),
        out_specs=P(ka, None, None, pb),
        check_vma=False,
    )
```

```python
import jax
import jax.numpy as jnp
import numpy as np
from jax import lax
from jax.experimental import pallas as pl
from jax.experimental.pallas import tpu as pltpu
from jax.sharding import Mesh
from jax.sharding import PartitionSpec as P

GRID = 32
BANDS = 4
OCC = 2
OWN = 2
PLANE = 8
ROWS = GRID * PLANE
CELLS = GRID**3
KPOINT_SCALING = 2.0
SCREENING_CUTOFF = 0.25
FIELD_ROWS = 32 * OWN
EXTRA = 8
PEERS = 32
PAIRS = [(0, 0, 0), (1, 1, 0), (0, 1, 0), (0, 1, 1), (2, 0, 0), (2, 0, 1), (3, 1, 0), (3, 1, 1)]


def phases(angle):
    turn = 2.0 * np.pi * (angle % GRID) / GRID
    return np.cos(turn), np.sin(turn)


def tables():
    row = np.arange(ROWS)
    lane = np.arange(128)
    hi, lo = row // PLANE, row % PLANE
    cos, sin = phases(hi[:, None] * hi[None] + 4 * lo[:, None] * lo[None])
    left = np.block([[cos, sin], [-sin, cos]])
    part, z = lane // GRID, lane % GRID
    cos, sin = phases(z[:, None] * z[None] + 8 * part[:, None] * part[None])
    right = np.block([[cos, -sin], [sin, cos]])
    twist = np.stack(phases(lo[:, None] * part[None]))
    return left.astype(jnp.bfloat16), right.astype(jnp.bfloat16), twist.astype(np.float32)


def wave_number(index):
    return ((index + GRID // 2) % GRID - GRID // 2).astype(jnp.float32)


def coulomb(offset, shift):
    row = lax.broadcasted_iota(jnp.int32, (ROWS, 128), 0)
    lane = lax.broadcasted_iota(jnp.int32, (ROWS, 128), 1)
    index = (row // PLANE, (lane // GRID) * PLANE + row % PLANE, lane % GRID)
    lattice = (offset // 16, offset // 4 % 4, offset % 4)
    squared = jnp.zeros((ROWS, 128), jnp.float32)
    for axis in range(3):
        moved = shift[axis].astype(jnp.float32) + lattice[axis].astype(jnp.float32) * 0.25
        component = wave_number(index[axis]) + moved
        squared += component * component
    return KPOINT_SCALING / (squared + SCREENING_CUTOFF)


def product(a, b):
    return jnp.dot(a, b, preferred_element_type=jnp.float32)


def coulomb_kernel(mine, theirs, kernel):
    place = mine[0, 4]
    for q in range(2):
        number = [jnp.where(place == q, mine[0, at], theirs[0, at]) for at in range(4)]
        kernel[q] = coulomb(number[0], number[1:]) * (1.0 / CELLS)


def apart_kernel(place, targets, parts, rows):
    for slot in range(BANDS):
        rows[...] = targets[band_of(slot, place[0, 0])].astype(jnp.float32)
        for part in range(2):
            parts[slot, part] = rows[pl.ds(part, ROWS, 2), :]


def band_of(slot, place):
    return 2 * place + slot if slot < OWN else slot - (1 + 2 * (slot - OWN)) * place


def exchange_kernel(core, kernel, targets, own, other, left, right, twist, out, rows, parts):
    for source, parity in ((own, core[0, 0]), (other, 1 - core[0, 0])):
        for q in range(2):
            for j in range(OCC):
                planes = source[16 * q : 16 * q + 16, 16 * j : 16 * j + 16].astype(jnp.float32)
                rows[q, j, :, pl.ds(parity, 1)] = planes[:, None]
    for q in range(2):
        for j in range(OCC):
            for part in range(2):
                parts[j, q, part] = rows[q, j, :, :, pl.ds(part, PLANE, 2), :].reshape(ROWS, 128)

    def twisted(re, im):
        return re * twist[0] + im * twist[1], im * twist[0] - re * twist[1]

    def density(band, j):
        tops, bottoms = [], []
        for q in range(2):
            re, im = parts[j, q, 0], parts[j, q, 1]
            tops.append(re * targets[band, 0] + im * targets[band, 1])
            bottoms.append(re * targets[band, 1] - im * targets[band, 0])
        return joined(tops, bottoms)

    def joined(tops, bottoms):
        rows = [jnp.concatenate(tops, 1), jnp.concatenate(bottoms, 1)]
        return jnp.concatenate(rows, 0).astype(jnp.bfloat16)

    def to_spectrum(blocks):
        pairs = []
        for q in range(2):
            cut = slice(128 * q, 128 * q + 128)
            pair = twisted(blocks[:ROWS, cut], blocks[ROWS:, cut])
            pairs.append(jnp.concatenate(pair, 1).astype(jnp.bfloat16))
        return product(jnp.concatenate(pairs, 0), right[...])

    def from_spectrum(spectrum):
        scaled = []
        for q in range(2):
            cut = slice(ROWS * q, ROWS * q + ROWS)
            pair = spectrum[cut, :128] * kernel[q], spectrum[cut, 128:] * -kernel[q]
            scaled.append(jnp.concatenate(pair, 1).astype(jnp.bfloat16))
        return product(jnp.concatenate(scaled, 0), right[...])

    def untwisted(back):
        tops, bottoms = [], []
        for q in range(2):
            cut = slice(ROWS * q, ROWS * q + ROWS)
            re, im = twisted(back[cut, :128], back[cut, 128:])
            tops.append(re)
            bottoms.append(im)
        return joined(tops, bottoms)

    def field(conjugates):
        re_sum, im_sum = None, None
        for j in range(OCC):
            for q in range(2):
                cut = slice(128 * q, 128 * q + 128)
                re, im = conjugates[j][:ROWS, cut], conjugates[j][ROWS:, cut]
                re_now = -(parts[j, q, 0] * re) - parts[j, q, 1] * im
                im_now = parts[j, q, 0] * im - parts[j, q, 1] * re
                re_sum = re_now if re_sum is None else re_sum + re_now
                im_sum = im_now if im_sum is None else im_sum + im_now
        return re_sum, im_sum

    units = [(band, j) for band in range(OWN) for j in range(OCC)]
    values = [product(left[...], density(*unit)) for unit in units]
    values = [to_spectrum(value) for value in values]
    values = [from_spectrum(value) for value in values]
    values = [product(left[...], untwisted(value)) for value in values]
    sums = {}
    for band in range(OWN):
        re, im = field(values[OCC * band : OCC * band + OCC])
        out[:, 32 * band : 32 * band + 16] = re.astype(jnp.bfloat16).reshape(16, 16, 128)
        out[:, 32 * band + 16 : 32 * band + 32] = im.astype(jnp.bfloat16).reshape(16, 16, 128)
        for slot, place, cross in PAIRS:
            if place == band:
                if cross:
                    total = targets[slot, 1] * re - targets[slot, 0] * im
                else:
                    total = targets[slot, 0] * re + targets[slot, 1] * im
                sums[slot, place, cross] = total.reshape(GRID, 8, 128).sum(0)
    value = jnp.concatenate([jnp.sum(sums[key], 0, keepdims=True) for key in PAIRS], 0)
    value = jnp.broadcast_to(jnp.sum(value, 1, keepdims=True), (8, 128))
    piece = lax.broadcasted_iota(jnp.int32, (8, 128), 1) // 32
    high = value.astype(jnp.bfloat16).astype(jnp.float32)
    middle = (value - high).astype(jnp.bfloat16).astype(jnp.float32)
    low = value - high - middle
    value = jnp.where(piece == 0, high, jnp.where(piece == 1, middle, jnp.where(piece == 2, low, 0.0)))
    out[:, FIELD_ROWS:] = jnp.broadcast_to(value.astype(jnp.bfloat16)[None], (16, EXTRA, 128))


def projector_kernel(shares, out):
    totals = []
    for group in range(2):
        total = shares[8 * group].astype(jnp.float32)
        for source in range(8 * group + 1, 8 * group + 8):
            total += shares[source].astype(jnp.float32)
        totals.append(total)
    value = {}
    for group in range(2):
        values = totals[group][FIELD_ROWS:]
        values = values + pltpu.roll(values, 96, 1) + pltpu.roll(values, 64, 1)
        values = values * (1.0 / CELLS)
        for at, (slot, own, cross) in enumerate(PAIRS):
            key = band_of(slot, group), band_of(own, group), cross
            value[key] = jnp.broadcast_to(values[at : at + 1, 0:1], (8, 128))

    def entry(row, column):
        i, j = row % BANDS, column % BANDS
        if row // BANDS == column // BANDS:
            return -(value[i, j, 0] if (i, j, 0) in value else value[j, i, 0])
        if i == j:
            return None
        return value[i, j, 1] if (i, j, 1) in value else -value[j, i, 1]

    size = 2 * BANDS
    factor, inverse = {}, {}
    for column in range(size):
        for row in range(column, size):
            rest = entry(row, column)
            for before in range(column):
                if (row, before) in factor and (column, before) in factor:
                    part = factor[row, before] * factor[column, before]
                    rest = -part if rest is None else rest - part
            if row == column:
                guess = lax.rsqrt(rest)
                inverse[row] = guess * (1.5 - 0.5 * rest * guess * guess)
            elif rest is not None:
                factor[row, column] = rest * inverse[column]
    solved = []
    for row in range(size):
        for_parts = []
        for part in range(2):
            band = row % BANDS
            at = 32 * (band % OWN) + 16 * (part if row < BANDS else 1 - part)
            rest = totals[band // OWN][at : at + 16].reshape(2, 8, 128)
            if row >= BANDS and part == 0:
                rest = -rest
            for before in range(row):
                if (row, before) in factor:
                    rest = rest - factor[row, before][None] * solved[before][part]
            rest = rest * inverse[row][None]
            for_parts.append(rest)
            out[pl.ds(32 * row + part, 16, 2), :] = rest.reshape(16, 128)
        solved.append(for_parts)


SMEM = pl.BlockSpec(memory_space=pltpu.SMEM)
VMEM = pl.BlockSpec(memory_space=pltpu.VMEM)


def call(kernel, name, shapes, specs, scratch, limit, *operands):
    return pl.pallas_call(
        kernel,
        out_shape=shapes,
        in_specs=specs,
        out_specs=jax.tree.map(lambda _: VMEM, shapes),
        scratch_shapes=scratch,
        compiler_params=pltpu.CompilerParams(vmem_limit_bytes=limit << 20),
        name=name,
    )(*operands)


def array(*shape, dtype=jnp.float32):
    return jax.ShapeDtypeStruct(shape, dtype)


def prepare(mine, theirs):
    return call(coulomb_kernel, "coulomb", array(2, ROWS, 128), [SMEM, SMEM], [], 2, mine, theirs)


def apart(place, targets):
    scratch = [pltpu.VMEM((2 * ROWS, 128), jnp.float32)]
    shape = array(BANDS, 2, ROWS, 128)
    return call(apart_kernel, "apart", shape, [SMEM, VMEM], scratch, 4, place, targets)


def exchange(*operands):
    scratch = [
        pltpu.VMEM((2, OCC, GRID // 2, 2, 2 * PLANE, 128), jnp.float32),
        pltpu.VMEM((OCC, 2, 2, ROWS, 128), jnp.float32),
    ]
    shape = array(16, FIELD_ROWS + EXTRA, 128, dtype=jnp.bfloat16)
    specs = [SMEM] + [VMEM] * (len(operands) - 1)
    return call(exchange_kernel, "exchange", shape, specs, scratch, 24, *operands)


def projector(shares):
    return call(projector_kernel, "projector", array(256, 128), [VMEM], [], 4, shares)


def interleaved(values):
    tiles = values.reshape(values.shape[0], 2, values.shape[2] // 128, 128)
    return jnp.swapaxes(tiles, 1, 2).reshape(values.shape[0], -1, 128)


def local(targets, partners, pair_map, shifts):
    left, right, twist = (jnp.asarray(table) for table in tables())
    core, group = (lax.axis_index(axis).reshape(1, 1) for axis in ("core", "xh"))
    plane = interleaved(partners[0]).reshape(1, 4 * PLANE, 128)
    operand = jnp.broadcast_to(plane, (PEERS, 4 * PLANE, 128))
    gathered = lax.all_to_all(operand, ("xh", "chip"), 0, 0, tiled=True)
    mine = jnp.concatenate([pair_map, shifts[0], group], 1)
    theirs = lax.ppermute(mine, "xh", [(0, 1), (1, 0)])
    parts = apart(group, interleaved(targets[0]))
    gathered, parts, theirs = lax.optimization_barrier((gathered, parts, theirs))
    swapped = lax.ppermute(gathered, "core", [(0, 1), (1, 0)])
    kernel = prepare(mine, theirs)
    shares = exchange(core, kernel, parts, gathered, swapped, left, right, twist)
    shares = lax.all_to_all(shares, ("xh", "zz"), 0, 0, tiled=True)
    rows = projector(shares).reshape(2 * BANDS, 16, 2, 128)
    return jnp.swapaxes(rows, 1, 2).reshape(1, 2 * BANDS, 2, 2048)


def solution(mesh):
    split = Mesh(mesh.devices.reshape(16, 2, 2, 8), ("chip", "core", "xh", "zz"))
    ka, pb = ("chip", "core"), ("xh", "zz")
    return jax.shard_map(
        local,
        mesh=split,
        in_specs=(
            P(ka, None, None, None),
            P(pb, None, None, ka),
            P(ka, pb),
            P(ka, pb, None),
        ),
        out_specs=P(ka, None, None, pb),
        check_vma=False,
    )
```

```python
import jax
import jax.numpy as jnp
import numpy as np
from jax import lax
from jax.experimental import pallas as pl
from jax.experimental.pallas import tpu as pltpu
from jax.sharding import Mesh
from jax.sharding import PartitionSpec as P


GRID = 32
BANDS = 4
OCC = 2
OWN = 2
PLANE = 8
ROWS = GRID * PLANE
CELLS = GRID**3
KPOINT_SCALING = 2.0
SCREENING_CUTOFF = 0.25
FIELD_ROWS = 32 * OWN
EXTRA = 8
PEERS = 32
PAIRS = [(0, 0, 0), (1, 1, 0), (0, 1, 0), (0, 1, 1), (2, 0, 0), (2, 0, 1), (3, 1, 0), (3, 1, 1)]


def phases(angle):
    turn = 2.0 * np.pi * (angle % GRID) / GRID
    return np.cos(turn), np.sin(turn)


def tables():
    row = np.arange(ROWS)
    lane = np.arange(128)
    hi, lo = row // PLANE, row % PLANE
    cos, sin = phases(hi[:, None] * hi[None] + 4 * lo[:, None] * lo[None])
    left = np.block([[cos, sin], [-sin, cos]])
    part, z = lane // GRID, lane % GRID
    cos, sin = phases(z[:, None] * z[None] + 8 * part[:, None] * part[None])
    right = np.block([[cos, -sin], [sin, cos]])
    twist = np.stack(phases(lo[:, None] * part[None]))
    return left.astype(jnp.bfloat16), right.astype(jnp.bfloat16), twist.astype(np.float32)


def wave_number(index):
    return ((index + GRID // 2) % GRID - GRID // 2).astype(jnp.float32)


def coulomb(offset, shift):
    row = lax.broadcasted_iota(jnp.int32, (ROWS, 128), 0)
    lane = lax.broadcasted_iota(jnp.int32, (ROWS, 128), 1)
    index = (row // PLANE, (lane // GRID) * PLANE + row % PLANE, lane % GRID)
    lattice = (offset // 16, offset // 4 % 4, offset % 4)
    squared = jnp.zeros((ROWS, 128), jnp.float32)
    for axis in range(3):
        moved = shift[axis].astype(jnp.float32) + lattice[axis].astype(jnp.float32) * 0.25
        component = wave_number(index[axis]) + moved
        squared += component * component
    return KPOINT_SCALING / (squared + SCREENING_CUTOFF)


def product(a, b):
    return jnp.dot(a, b, preferred_element_type=jnp.float32)


def coulomb_kernel(mine, theirs, kernel):
    place = mine[0, 4]
    for q in range(2):
        number = [jnp.where(place == q, mine[0, at], theirs[0, at]) for at in range(4)]
        kernel[q] = coulomb(number[0], number[1:]) * (1.0 / CELLS)


def apart_kernel(place, targets, parts, rows):
    for slot in range(BANDS):
        rows[...] = targets[band_of(slot, place[0, 0])].astype(jnp.float32)
        for part in range(2):
            parts[slot, part] = rows[pl.ds(part, ROWS, 2), :]


def band_of(slot, place):
    return 2 * place + slot if slot < OWN else slot - (1 + 2 * (slot - OWN)) * place


def exchange_kernel(core, kernel, targets, own, other, left, right, twist, out, rows, parts):
    for source, parity in ((own, core[0, 0]), (other, 1 - core[0, 0])):
        for q in range(2):
            for j in range(OCC):
                planes = source[16 * q : 16 * q + 16, 16 * j : 16 * j + 16].astype(jnp.float32)
                rows[q, j, :, pl.ds(parity, 1)] = planes[:, None]
    for q in range(2):
        for j in range(OCC):
            for part in range(2):
                parts[j, q, part] = rows[q, j, :, :, pl.ds(part, PLANE, 2), :].reshape(ROWS, 128)

    def twisted(re, im):
        return re * twist[0] + im * twist[1], im * twist[0] - re * twist[1]

    def density(band, j):
        tops, bottoms = [], []
        for q in range(2):
            re, im = parts[j, q, 0], parts[j, q, 1]
            tops.append(re * targets[band, 0] + im * targets[band, 1])
            bottoms.append(re * targets[band, 1] - im * targets[band, 0])
        return joined(tops, bottoms)

    def joined(tops, bottoms):
        rows = [jnp.concatenate(tops, 1), jnp.concatenate(bottoms, 1)]
        return jnp.concatenate(rows, 0).astype(jnp.bfloat16)

    def to_spectrum(blocks):
        pairs = []
        for q in range(2):
            cut = slice(128 * q, 128 * q + 128)
            pair = twisted(blocks[:ROWS, cut], blocks[ROWS:, cut])
            pairs.append(jnp.concatenate(pair, 1).astype(jnp.bfloat16))
        return product(jnp.concatenate(pairs, 0), right[...])

    def from_spectrum(spectrum):
        scaled = []
        for q in range(2):
            cut = slice(ROWS * q, ROWS * q + ROWS)
            pair = spectrum[cut, :128] * kernel[q], spectrum[cut, 128:] * -kernel[q]
            scaled.append(jnp.concatenate(pair, 1).astype(jnp.bfloat16))
        return product(jnp.concatenate(scaled, 0), right[...])

    def untwisted(back):
        tops, bottoms = [], []
        for q in range(2):
            cut = slice(ROWS * q, ROWS * q + ROWS)
            re, im = twisted(back[cut, :128], back[cut, 128:])
            tops.append(re)
            bottoms.append(im)
        return joined(tops, bottoms)

    def field(conjugates):
        re_sum, im_sum = None, None
        for j in range(OCC):
            for q in range(2):
                cut = slice(128 * q, 128 * q + 128)
                re, im = conjugates[j][:ROWS, cut], conjugates[j][ROWS:, cut]
                re_now = -(parts[j, q, 0] * re) - parts[j, q, 1] * im
                im_now = parts[j, q, 0] * im - parts[j, q, 1] * re
                re_sum = re_now if re_sum is None else re_sum + re_now
                im_sum = im_now if im_sum is None else im_sum + im_now
        return re_sum, im_sum

    units = [(band, j) for band in range(OWN) for j in range(OCC)]
    values = [product(left[...], density(*unit)) for unit in units]
    values = [to_spectrum(value) for value in values]
    values = [from_spectrum(value) for value in values]
    values = [product(left[...], untwisted(value)) for value in values]
    sums = {}
    for band in range(OWN):
        re, im = field(values[OCC * band : OCC * band + OCC])
        out[:, 32 * band : 32 * band + 16] = re.astype(jnp.bfloat16).reshape(16, 16, 128)
        out[:, 32 * band + 16 : 32 * band + 32] = im.astype(jnp.bfloat16).reshape(16, 16, 128)
        for slot, place, cross in PAIRS:
            if place == band:
                if cross:
                    total = targets[slot, 1] * re - targets[slot, 0] * im
                else:
                    total = targets[slot, 0] * re + targets[slot, 1] * im
                sums[slot, place, cross] = total.reshape(GRID, 8, 128).sum(0)
    value = jnp.concatenate([jnp.sum(sums[key], 0, keepdims=True) for key in PAIRS], 0)
    value = jnp.broadcast_to(jnp.sum(value, 1, keepdims=True), (8, 128))
    piece = lax.broadcasted_iota(jnp.int32, (8, 128), 1) // 32
    high = value.astype(jnp.bfloat16).astype(jnp.float32)
    middle = (value - high).astype(jnp.bfloat16).astype(jnp.float32)
    low = value - high - middle
    value = jnp.where(piece == 0, high, jnp.where(piece == 1, middle, jnp.where(piece == 2, low, 0.0)))
    out[:, FIELD_ROWS:] = jnp.broadcast_to(value.astype(jnp.bfloat16)[None], (16, EXTRA, 128))


def projector_kernel(shares, out):
    totals = []
    for group in range(2):
        total = shares[8 * group].astype(jnp.float32)
        for source in range(8 * group + 1, 8 * group + 8):
            total += shares[source].astype(jnp.float32)
        totals.append(total)
    value = {}
    for group in range(2):
        values = totals[group][FIELD_ROWS:]
        values = values + pltpu.roll(values, 96, 1) + pltpu.roll(values, 64, 1)
        values = values * (1.0 / CELLS)
        for at, (slot, own, cross) in enumerate(PAIRS):
            key = band_of(slot, group), band_of(own, group), cross
            value[key] = jnp.broadcast_to(values[at : at + 1, 0:1], (8, 128))

    def entry(row, column):
        i, j = row % BANDS, column % BANDS
        if row // BANDS == column // BANDS:
            return -(value[i, j, 0] if (i, j, 0) in value else value[j, i, 0])
        if i == j:
            return None
        return value[i, j, 1] if (i, j, 1) in value else -value[j, i, 1]

    size = 2 * BANDS
    factor, inverse = {}, {}
    for column in range(size):
        for row in range(column, size):
            rest = entry(row, column)
            for before in range(column):
                if (row, before) in factor and (column, before) in factor:
                    part = factor[row, before] * factor[column, before]
                    rest = -part if rest is None else rest - part
            if row == column:
                guess = lax.rsqrt(rest)
                inverse[row] = guess * (1.5 - 0.5 * rest * guess * guess)
            elif rest is not None:
                factor[row, column] = rest * inverse[column]
    solved = []
    for row in range(size):
        for_parts = []
        for part in range(2):
            band = row % BANDS
            at = 32 * (band % OWN) + 16 * (part if row < BANDS else 1 - part)
            rest = totals[band // OWN][at : at + 16].reshape(2, 8, 128)
            if row >= BANDS and part == 0:
                rest = -rest
            for before in range(row):
                if (row, before) in factor:
                    rest = rest - factor[row, before][None] * solved[before][part]
            rest = rest * inverse[row][None]
            for_parts.append(rest)
            out[pl.ds(32 * row + part, 16, 2), :] = rest.reshape(16, 128)
        solved.append(for_parts)


SMEM = pl.BlockSpec(memory_space=pltpu.SMEM)
VMEM = pl.BlockSpec(memory_space=pltpu.VMEM)


def call(kernel, shapes, specs, scratch, limit, *operands):
    return pl.pallas_call(
        kernel,
        out_shape=shapes,
        in_specs=specs,
        out_specs=jax.tree.map(lambda _: VMEM, shapes),
        scratch_shapes=scratch,
        compiler_params=pltpu.CompilerParams(vmem_limit_bytes=limit << 20),
    )(*operands)


def array(*shape, dtype=jnp.float32):
    return jax.ShapeDtypeStruct(shape, dtype)


def prepare(mine, theirs):
    return call(coulomb_kernel, array(2, ROWS, 128), [SMEM, SMEM], [], 2, mine, theirs)


def apart(place, targets):
    scratch = [pltpu.VMEM((2 * ROWS, 128), jnp.float32)]
    shape = array(BANDS, 2, ROWS, 128)
    return call(apart_kernel, shape, [SMEM, VMEM], scratch, 4, place, targets)


def exchange(*operands):
    scratch = [
        pltpu.VMEM((2, OCC, GRID // 2, 2, 2 * PLANE, 128), jnp.float32),
        pltpu.VMEM((OCC, 2, 2, ROWS, 128), jnp.float32),
    ]
    shape = array(16, FIELD_ROWS + EXTRA, 128, dtype=jnp.bfloat16)
    specs = [SMEM] + [VMEM] * (len(operands) - 1)
    return call(exchange_kernel, shape, specs, scratch, 24, *operands)


def projector(shares):
    return call(projector_kernel, array(256, 128), [VMEM], [], 4, shares)


def interleaved(values):
    tiles = values.reshape(values.shape[0], 2, values.shape[2] // 128, 128)
    return jnp.swapaxes(tiles, 1, 2).reshape(values.shape[0], -1, 128)


def local(targets, partners, pair_map, shifts):
    left, right, twist = (jnp.asarray(table) for table in tables())
    core, group = (lax.axis_index(axis).reshape(1, 1) for axis in ("core", "xh"))
    plane = interleaved(partners[0]).reshape(1, 4 * PLANE, 128)
    operand = jnp.broadcast_to(plane, (PEERS, 4 * PLANE, 128))
    gathered = lax.all_to_all(operand, ("xh", "chip"), 0, 0, tiled=True)
    mine = jnp.concatenate([pair_map, shifts[0], group], 1)
    theirs = lax.ppermute(mine, "xh", [(0, 1), (1, 0)])
    parts = apart(group, interleaved(targets[0]))
    gathered, parts = lax.optimization_barrier((gathered, parts))
    swapped = lax.ppermute(gathered, "core", [(0, 1), (1, 0)])
    kernel = prepare(mine, theirs)
    shares = exchange(core, kernel, parts, gathered, swapped, left, right, twist)
    shares = lax.all_to_all(shares, ("xh", "zz"), 0, 0, tiled=True)
    rows = projector(shares).reshape(2 * BANDS, 16, 2, 128)
    return jnp.swapaxes(rows, 1, 2).reshape(1, 2 * BANDS, 2, 2048)


def solution(mesh):
    split = Mesh(mesh.devices.reshape(16, 2, 2, 8), ("chip", "core", "xh", "zz"))
    ka, pb = ("chip", "core"), ("xh", "zz")
    return jax.shard_map(
        local,
        mesh=split,
        in_specs=(
            P(ka, None, None, None),
            P(pb, None, None, ka),
            P(ka, pb),
            P(ka, pb, None),
        ),
        out_specs=P(ka, None, None, pb),
        check_vma=False,
    )
```

```python
import jax
import jax.numpy as jnp
import numpy as np
from jax import lax
from jax.experimental import pallas as pl
from jax.experimental.pallas import tpu as pltpu
from jax.sharding import Mesh
from jax.sharding import PartitionSpec as P

GRID = 32
BANDS = 4
OCC = 2
OWN = 2
PLANE = 8
ROWS = GRID * PLANE
CELLS = GRID**3
KPOINT_SCALING = 2.0
SCREENING_CUTOFF = 0.25
FIELD_ROWS = 32 * OWN
EXTRA = 8
PEERS = 32
PLANE_FIRST = 20
SUM_FIRST = 12
PAIRS = [(0, 0, 0), (1, 1, 0), (0, 1, 0), (0, 1, 1), (2, 0, 0), (2, 0, 1), (3, 1, 0), (3, 1, 1)]


def phases(angle):
    turn = 2.0 * np.pi * (angle % GRID) / GRID
    return np.cos(turn), np.sin(turn)


def tables():
    row = np.arange(ROWS)
    lane = np.arange(128)
    hi, lo = row // PLANE, row % PLANE
    cos, sin = phases(hi[:, None] * hi[None] + 4 * lo[:, None] * lo[None])
    left = np.block([[cos, sin], [-sin, cos]])
    part, z = lane // GRID, lane % GRID
    cos, sin = phases(z[:, None] * z[None] + 8 * part[:, None] * part[None])
    right = np.block([[cos, -sin], [sin, cos]])
    twist = np.stack(phases(lo[:, None] * part[None]))
    return left.astype(jnp.bfloat16), right.astype(jnp.bfloat16), twist.astype(np.float32)


def wave_number(index):
    return ((index + GRID // 2) % GRID - GRID // 2).astype(jnp.float32)


def coulomb(offset, shift):
    row = lax.broadcasted_iota(jnp.int32, (ROWS, 128), 0)
    lane = lax.broadcasted_iota(jnp.int32, (ROWS, 128), 1)
    index = (row // PLANE, (lane // GRID) * PLANE + row % PLANE, lane % GRID)
    lattice = (offset // 16, offset // 4 % 4, offset % 4)
    squared = jnp.zeros((ROWS, 128), jnp.float32)
    for axis in range(3):
        moved = shift[axis].astype(jnp.float32) + lattice[axis].astype(jnp.float32) * 0.25
        component = wave_number(index[axis]) + moved
        squared += component * component
    return KPOINT_SCALING / (squared + SCREENING_CUTOFF)


def order(count, first):
    return [[at ^ first for at in range(count)]]


def product(a, b):
    return jnp.dot(a, b, preferred_element_type=jnp.float32)


def coulomb_kernel(mine, theirs, kernel):
    place = mine[0, 4]
    for q in range(2):
        number = [jnp.where(place == q, mine[0, at], theirs[0, at]) for at in range(4)]
        kernel[q] = coulomb(number[0], number[1:]) * (1.0 / CELLS)


def apart_kernel(place, targets, parts, rows):
    for slot in range(BANDS):
        rows[...] = targets[band_of(slot, place[0, 0])].astype(jnp.float32)
        for part in range(2):
            parts[slot, part] = rows[pl.ds(part, ROWS, 2), :]


def band_of(slot, place):
    return 2 * place + slot if slot < OWN else slot - (1 + 2 * (slot - OWN)) * place


def exchange_kernel(core, kernel, targets, own, other, left, right, twist, out, rows, parts):
    for source, parity in ((own, core[0, 0]), (other, 1 - core[0, 0])):
        for q in range(2):
            for j in range(OCC):
                for m in range(0, 16, 4):
                    at = (16 * q + m) ^ PLANE_FIRST
                    planes = source[at : at + 4, 16 * j : 16 * j + 16].astype(jnp.float32)
                    rows[q, j, m : m + 4, pl.ds(parity, 1)] = planes[:, None]
    for q in range(2):
        for j in range(OCC):
            for part in range(2):
                parts[j, q, part] = rows[q, j, :, :, pl.ds(part, PLANE, 2), :].reshape(ROWS, 128)

    def twisted(re, im):
        return re * twist[0] + im * twist[1], im * twist[0] - re * twist[1]

    def density(band, j):
        tops, bottoms = [], []
        for q in range(2):
            re, im = parts[j, q, 0], parts[j, q, 1]
            tops.append(re * targets[band, 0] + im * targets[band, 1])
            bottoms.append(re * targets[band, 1] - im * targets[band, 0])
        return joined(tops, bottoms)

    def joined(tops, bottoms):
        rows = [jnp.concatenate(tops, 1), jnp.concatenate(bottoms, 1)]
        return jnp.concatenate(rows, 0).astype(jnp.bfloat16)

    def to_spectrum(blocks):
        pairs = []
        for q in range(2):
            cut = slice(128 * q, 128 * q + 128)
            pair = twisted(blocks[:ROWS, cut], blocks[ROWS:, cut])
            pairs.append(jnp.concatenate(pair, 1).astype(jnp.bfloat16))
        return product(jnp.concatenate(pairs, 0), right[...])

    def from_spectrum(spectrum):
        scaled = []
        for q in range(2):
            cut = slice(ROWS * q, ROWS * q + ROWS)
            pair = spectrum[cut, :128] * kernel[q], spectrum[cut, 128:] * -kernel[q]
            scaled.append(jnp.concatenate(pair, 1).astype(jnp.bfloat16))
        return product(jnp.concatenate(scaled, 0), right[...])

    def untwisted(back):
        tops, bottoms = [], []
        for q in range(2):
            cut = slice(ROWS * q, ROWS * q + ROWS)
            re, im = twisted(back[cut, :128], back[cut, 128:])
            tops.append(re)
            bottoms.append(im)
        return joined(tops, bottoms)

    def field(conjugates):
        re_sum, im_sum = None, None
        for j in range(OCC):
            for q in range(2):
                cut = slice(128 * q, 128 * q + 128)
                re, im = conjugates[j][:ROWS, cut], conjugates[j][ROWS:, cut]
                re_now = -(parts[j, q, 0] * re) - parts[j, q, 1] * im
                im_now = parts[j, q, 0] * im - parts[j, q, 1] * re
                re_sum = re_now if re_sum is None else re_sum + re_now
                im_sum = im_now if im_sum is None else im_sum + im_now
        return re_sum, im_sum

    units = [(band, j) for band in range(OWN) for j in range(OCC)]
    values = [product(left[...], density(*unit)) for unit in units]
    values = [to_spectrum(value) for value in values]
    values = [from_spectrum(value) for value in values]
    values = [product(left[...], untwisted(value)) for value in values]
    sums = {}
    for band in range(OWN):
        re, im = field(values[OCC * band : OCC * band + OCC])
        for part, value in enumerate((re, im)):
            value = value.astype(jnp.bfloat16).reshape(16, 16, 128)
            first = 32 * band + 16 * part
            for to in range(0, 16, 4):
                at = to ^ SUM_FIRST
                out[at : at + 4, first : first + 16] = value[to : to + 4]
        for slot, place, cross in PAIRS:
            if place == band:
                if cross:
                    total = targets[slot, 1] * re - targets[slot, 0] * im
                else:
                    total = targets[slot, 0] * re + targets[slot, 1] * im
                sums[slot, place, cross] = total.reshape(GRID, 8, 128).sum(0)
    value = jnp.concatenate([jnp.sum(sums[key], 0, keepdims=True) for key in PAIRS], 0)
    value = jnp.broadcast_to(jnp.sum(value, 1, keepdims=True), (8, 128))
    piece = lax.broadcasted_iota(jnp.int32, (8, 128), 1) // 32
    high = value.astype(jnp.bfloat16).astype(jnp.float32)
    middle = (value - high).astype(jnp.bfloat16).astype(jnp.float32)
    low = value - high - middle
    value = jnp.where(piece == 0, high, jnp.where(piece == 1, middle, jnp.where(piece == 2, low, 0.0)))
    out[:, FIELD_ROWS:] = jnp.broadcast_to(value.astype(jnp.bfloat16)[None], (16, EXTRA, 128))


def projector_kernel(shares, out):
    totals = []
    for group in range(2):
        total = shares[(8 * group) ^ SUM_FIRST].astype(jnp.float32)
        for source in range(8 * group + 1, 8 * group + 8):
            total += shares[source ^ SUM_FIRST].astype(jnp.float32)
        totals.append(total)
    value = {}
    for group in range(2):
        values = totals[group][FIELD_ROWS:]
        values = values + pltpu.roll(values, 96, 1) + pltpu.roll(values, 64, 1)
        values = values * (1.0 / CELLS)
        for at, (slot, own, cross) in enumerate(PAIRS):
            key = band_of(slot, group), band_of(own, group), cross
            value[key] = jnp.broadcast_to(values[at : at + 1, 0:1], (8, 128))

    def entry(row, column):
        i, j = row % BANDS, column % BANDS
        if row // BANDS == column // BANDS:
            return -(value[i, j, 0] if (i, j, 0) in value else value[j, i, 0])
        if i == j:
            return None
        return value[i, j, 1] if (i, j, 1) in value else -value[j, i, 1]

    size = 2 * BANDS
    factor, inverse = {}, {}
    for column in range(size):
        for row in range(column, size):
            rest = entry(row, column)
            for before in range(column):
                if (row, before) in factor and (column, before) in factor:
                    part = factor[row, before] * factor[column, before]
                    rest = -part if rest is None else rest - part
            if row == column:
                guess = lax.rsqrt(rest)
                inverse[row] = guess * (1.5 - 0.5 * rest * guess * guess)
            elif rest is not None:
                factor[row, column] = rest * inverse[column]
    solved = []
    for row in range(size):
        for_parts = []
        for part in range(2):
            band = row % BANDS
            at = 32 * (band % OWN) + 16 * (part if row < BANDS else 1 - part)
            rest = totals[band // OWN][at : at + 16].reshape(2, 8, 128)
            if row >= BANDS and part == 0:
                rest = -rest
            for before in range(row):
                if (row, before) in factor:
                    rest = rest - factor[row, before][None] * solved[before][part]
            rest = rest * inverse[row][None]
            for_parts.append(rest)
            out[pl.ds(32 * row + part, 16, 2), :] = rest.reshape(16, 128)
        solved.append(for_parts)


SMEM = pl.BlockSpec(memory_space=pltpu.SMEM)
VMEM = pl.BlockSpec(memory_space=pltpu.VMEM)


def call(kernel, name, shapes, specs, scratch, limit, *operands):
    return pl.pallas_call(
        kernel,
        out_shape=shapes,
        in_specs=specs,
        out_specs=jax.tree.map(lambda _: VMEM, shapes),
        scratch_shapes=scratch,
        compiler_params=pltpu.CompilerParams(vmem_limit_bytes=limit << 20),
        name=name,
    )(*operands)


def array(*shape, dtype=jnp.float32):
    return jax.ShapeDtypeStruct(shape, dtype)


def prepare(mine, theirs):
    return call(coulomb_kernel, "coulomb", array(2, ROWS, 128), [SMEM, SMEM], [], 2, mine, theirs)


def apart(place, targets):
    scratch = [pltpu.VMEM((2 * ROWS, 128), jnp.float32)]
    shape = array(BANDS, 2, ROWS, 128)
    return call(apart_kernel, "apart", shape, [SMEM, VMEM], scratch, 4, place, targets)


def exchange(*operands):
    scratch = [
        pltpu.VMEM((2, OCC, GRID // 2, 2, 2 * PLANE, 128), jnp.float32),
        pltpu.VMEM((OCC, 2, 2, ROWS, 128), jnp.float32),
    ]
    shape = array(16, FIELD_ROWS + EXTRA, 128, dtype=jnp.bfloat16)
    specs = [SMEM] + [VMEM] * (len(operands) - 1)
    return call(exchange_kernel, "exchange", shape, specs, scratch, 24, *operands)


def projector(shares):
    return call(projector_kernel, "projector", array(256, 128), [VMEM], [], 4, shares)


def interleaved(values):
    tiles = values.reshape(values.shape[0], 2, values.shape[2] // 128, 128)
    return jnp.swapaxes(tiles, 1, 2).reshape(values.shape[0], -1, 128)


def local(targets, partners, pair_map, shifts):
    left, right, twist = (jnp.asarray(table) for table in tables())
    core, group = (lax.axis_index(axis).reshape(1, 1) for axis in ("core", "xh"))
    plane = interleaved(partners[0]).reshape(1, 4 * PLANE, 128)
    operand = jnp.broadcast_to(plane, (PEERS, 4 * PLANE, 128))
    gathered = lax.all_to_all(
        operand, ("xh", "chip"), 0, 0, axis_index_groups=order(PEERS, PLANE_FIRST), tiled=True
    )
    mine = jnp.concatenate([pair_map, shifts[0], group], 1)
    theirs = lax.ppermute(mine, "xh", [(0, 1), (1, 0)])
    parts = apart(group, interleaved(targets[0]))
    gathered, parts, theirs = lax.optimization_barrier((gathered, parts, theirs))
    swapped = lax.ppermute(gathered, "core", [(0, 1), (1, 0)])
    kernel = prepare(mine, theirs)
    shares = exchange(core, kernel, parts, gathered, swapped, left, right, twist)
    shares = lax.all_to_all(
        shares, ("xh", "zz"), 0, 0, axis_index_groups=order(16, SUM_FIRST), tiled=True
    )
    rows = projector(shares).reshape(2 * BANDS, 16, 2, 128)
    return jnp.swapaxes(rows, 1, 2).reshape(1, 2 * BANDS, 2, 2048)


def solution(mesh):
    split = Mesh(mesh.devices.reshape(16, 2, 2, 8), ("chip", "core", "xh", "zz"))
    ka, pb = ("chip", "core"), ("xh", "zz")
    return jax.shard_map(
        local,
        mesh=split,
        in_specs=(
            P(ka, None, None, None),
            P(pb, None, None, ka),
            P(ka, pb),
            P(ka, pb, None),
        ),
        out_specs=P(ka, None, None, pb),
        check_vma=False,
    )
```

```python
import jax
import jax.numpy as jnp
import numpy as np
from jax import lax
from jax.experimental import pallas as pl
from jax.experimental.pallas import tpu as pltpu
from jax.sharding import Mesh
from jax.sharding import PartitionSpec as P


GRID = 32
BANDS = 4
OCC = 2
OWN = 2
PLANE = 8
ROWS = GRID * PLANE
CELLS = GRID**3
KPOINT_SCALING = 2.0
SCREENING_CUTOFF = 0.25
FIELD_ROWS = 32 * OWN
EXTRA = 8
PEERS = 32
PLANE_FIRST = 20
SUM_FIRST = 12
PAIRS = [(0, 0, 0), (1, 1, 0), (0, 1, 0), (0, 1, 1), (2, 0, 0), (2, 0, 1), (3, 1, 0), (3, 1, 1)]


def phases(angle):
    turn = 2.0 * np.pi * (angle % GRID) / GRID
    return np.cos(turn), np.sin(turn)


def tables():
    row = np.arange(ROWS)
    lane = np.arange(128)
    hi, lo = row // PLANE, row % PLANE
    cos, sin = phases(hi[:, None] * hi[None] + 4 * lo[:, None] * lo[None])
    left = np.block([[cos, sin], [-sin, cos]])
    part, z = lane // GRID, lane % GRID
    cos, sin = phases(z[:, None] * z[None] + 8 * part[:, None] * part[None])
    right = np.block([[cos, -sin], [sin, cos]])
    twist = np.stack(phases(lo[:, None] * part[None]))
    return left.astype(jnp.bfloat16), right.astype(jnp.bfloat16), twist.astype(np.float32)


def wave_number(index):
    return ((index + GRID // 2) % GRID - GRID // 2).astype(jnp.float32)


def coulomb(offset, shift):
    row = lax.broadcasted_iota(jnp.int32, (ROWS, 128), 0)
    lane = lax.broadcasted_iota(jnp.int32, (ROWS, 128), 1)
    index = (row // PLANE, (lane // GRID) * PLANE + row % PLANE, lane % GRID)
    lattice = (offset // 16, offset // 4 % 4, offset % 4)
    squared = jnp.zeros((ROWS, 128), jnp.float32)
    for axis in range(3):
        moved = shift[axis].astype(jnp.float32) + lattice[axis].astype(jnp.float32) * 0.25
        component = wave_number(index[axis]) + moved
        squared += component * component
    return KPOINT_SCALING / (squared + SCREENING_CUTOFF)


def order(count, first):
    return [[at ^ first for at in range(count)]]


def product(a, b):
    return jnp.dot(a, b, preferred_element_type=jnp.float32)


def coulomb_kernel(mine, theirs, kernel):
    place = mine[0, 4]
    for q in range(2):
        number = [jnp.where(place == q, mine[0, at], theirs[0, at]) for at in range(4)]
        kernel[q] = coulomb(number[0], number[1:]) * (1.0 / CELLS)


def apart_kernel(place, targets, parts, rows):
    for slot in range(BANDS):
        rows[...] = targets[band_of(slot, place[0, 0])].astype(jnp.float32)
        for part in range(2):
            parts[slot, part] = rows[pl.ds(part, ROWS, 2), :]


def band_of(slot, place):
    return 2 * place + slot if slot < OWN else slot - (1 + 2 * (slot - OWN)) * place


def exchange_kernel(core, kernel, targets, own, other, left, right, twist, out, rows, parts):
    for source, parity in ((own, core[0, 0]), (other, 1 - core[0, 0])):
        for q in range(2):
            for j in range(OCC):
                for m in range(0, 16, 4):
                    at = (16 * q + m) ^ PLANE_FIRST
                    planes = source[at : at + 4, 16 * j : 16 * j + 16].astype(jnp.float32)
                    rows[q, j, m : m + 4, pl.ds(parity, 1)] = planes[:, None]
    for q in range(2):
        for j in range(OCC):
            for part in range(2):
                parts[j, q, part] = rows[q, j, :, :, pl.ds(part, PLANE, 2), :].reshape(ROWS, 128)

    def twisted(re, im):
        return re * twist[0] + im * twist[1], im * twist[0] - re * twist[1]

    def density(band, j):
        tops, bottoms = [], []
        for q in range(2):
            re, im = parts[j, q, 0], parts[j, q, 1]
            tops.append(re * targets[band, 0] + im * targets[band, 1])
            bottoms.append(re * targets[band, 1] - im * targets[band, 0])
        return joined(tops, bottoms)

    def joined(tops, bottoms):
        rows = [jnp.concatenate(tops, 1), jnp.concatenate(bottoms, 1)]
        return jnp.concatenate(rows, 0).astype(jnp.bfloat16)

    def to_spectrum(blocks):
        pairs = []
        for q in range(2):
            cut = slice(128 * q, 128 * q + 128)
            pair = twisted(blocks[:ROWS, cut], blocks[ROWS:, cut])
            pairs.append(jnp.concatenate(pair, 1).astype(jnp.bfloat16))
        return product(jnp.concatenate(pairs, 0), right[...])

    def from_spectrum(spectrum):
        scaled = []
        for q in range(2):
            cut = slice(ROWS * q, ROWS * q + ROWS)
            pair = spectrum[cut, :128] * kernel[q], spectrum[cut, 128:] * -kernel[q]
            scaled.append(jnp.concatenate(pair, 1).astype(jnp.bfloat16))
        return product(jnp.concatenate(scaled, 0), right[...])

    def untwisted(back):
        tops, bottoms = [], []
        for q in range(2):
            cut = slice(ROWS * q, ROWS * q + ROWS)
            re, im = twisted(back[cut, :128], back[cut, 128:])
            tops.append(re)
            bottoms.append(im)
        return joined(tops, bottoms)

    def field(conjugates):
        re_sum, im_sum = None, None
        for j in range(OCC):
            for q in range(2):
                cut = slice(128 * q, 128 * q + 128)
                re, im = conjugates[j][:ROWS, cut], conjugates[j][ROWS:, cut]
                re_now = -(parts[j, q, 0] * re) - parts[j, q, 1] * im
                im_now = parts[j, q, 0] * im - parts[j, q, 1] * re
                re_sum = re_now if re_sum is None else re_sum + re_now
                im_sum = im_now if im_sum is None else im_sum + im_now
        return re_sum, im_sum

    units = [(band, j) for band in range(OWN) for j in range(OCC)]
    values = [product(left[...], density(*unit)) for unit in units]
    values = [to_spectrum(value) for value in values]
    values = [from_spectrum(value) for value in values]
    values = [product(left[...], untwisted(value)) for value in values]
    sums = {}
    for band in range(OWN):
        re, im = field(values[OCC * band : OCC * band + OCC])
        for part, value in enumerate((re, im)):
            value = value.astype(jnp.bfloat16).reshape(16, 16, 128)
            first = 32 * band + 16 * part
            for to in range(0, 16, 4):
                at = to ^ SUM_FIRST
                out[at : at + 4, first : first + 16] = value[to : to + 4]
        for slot, place, cross in PAIRS:
            if place == band:
                if cross:
                    total = targets[slot, 1] * re - targets[slot, 0] * im
                else:
                    total = targets[slot, 0] * re + targets[slot, 1] * im
                sums[slot, place, cross] = total.reshape(GRID, 8, 128).sum(0)
    value = jnp.concatenate([jnp.sum(sums[key], 0, keepdims=True) for key in PAIRS], 0)
    value = jnp.broadcast_to(jnp.sum(value, 1, keepdims=True), (8, 128))
    piece = lax.broadcasted_iota(jnp.int32, (8, 128), 1) // 32
    high = value.astype(jnp.bfloat16).astype(jnp.float32)
    middle = (value - high).astype(jnp.bfloat16).astype(jnp.float32)
    low = value - high - middle
    value = jnp.where(piece == 0, high, jnp.where(piece == 1, middle, jnp.where(piece == 2, low, 0.0)))
    out[:, FIELD_ROWS:] = jnp.broadcast_to(value.astype(jnp.bfloat16)[None], (16, EXTRA, 128))


def projector_kernel(shares, out):
    totals = []
    for group in range(2):
        total = shares[(8 * group) ^ SUM_FIRST].astype(jnp.float32)
        for source in range(8 * group + 1, 8 * group + 8):
            total += shares[source ^ SUM_FIRST].astype(jnp.float32)
        totals.append(total)
    value = {}
    for group in range(2):
        values = totals[group][FIELD_ROWS:]
        values = values + pltpu.roll(values, 96, 1) + pltpu.roll(values, 64, 1)
        values = values * (1.0 / CELLS)
        for at, (slot, own, cross) in enumerate(PAIRS):
            key = band_of(slot, group), band_of(own, group), cross
            value[key] = jnp.broadcast_to(values[at : at + 1, 0:1], (8, 128))

    def entry(row, column):
        i, j = row % BANDS, column % BANDS
        if row // BANDS == column // BANDS:
            return -(value[i, j, 0] if (i, j, 0) in value else value[j, i, 0])
        if i == j:
            return None
        return value[i, j, 1] if (i, j, 1) in value else -value[j, i, 1]

    size = 2 * BANDS
    factor, inverse = {}, {}
    for column in range(size):
        for row in range(column, size):
            rest = entry(row, column)
            for before in range(column):
                if (row, before) in factor and (column, before) in factor:
                    part = factor[row, before] * factor[column, before]
                    rest = -part if rest is None else rest - part
            if row == column:
                guess = lax.rsqrt(rest)
                inverse[row] = guess * (1.5 - 0.5 * rest * guess * guess)
            elif rest is not None:
                factor[row, column] = rest * inverse[column]
    solved = []
    for row in range(size):
        for_parts = []
        for part in range(2):
            band = row % BANDS
            at = 32 * (band % OWN) + 16 * (part if row < BANDS else 1 - part)
            rest = totals[band // OWN][at : at + 16].reshape(2, 8, 128)
            if row >= BANDS and part == 0:
                rest = -rest
            for before in range(row):
                if (row, before) in factor:
                    rest = rest - factor[row, before][None] * solved[before][part]
            rest = rest * inverse[row][None]
            for_parts.append(rest)
            out[pl.ds(32 * row + part, 16, 2), :] = rest.reshape(16, 128)
        solved.append(for_parts)


SMEM = pl.BlockSpec(memory_space=pltpu.SMEM)
VMEM = pl.BlockSpec(memory_space=pltpu.VMEM)


def call(kernel, shapes, specs, scratch, limit, *operands):
    return pl.pallas_call(
        kernel,
        out_shape=shapes,
        in_specs=specs,
        out_specs=jax.tree.map(lambda _: VMEM, shapes),
        scratch_shapes=scratch,
        compiler_params=pltpu.CompilerParams(vmem_limit_bytes=limit << 20),
    )(*operands)


def array(*shape, dtype=jnp.float32):
    return jax.ShapeDtypeStruct(shape, dtype)


def prepare(mine, theirs):
    return call(coulomb_kernel, array(2, ROWS, 128), [SMEM, SMEM], [], 2, mine, theirs)


def apart(place, targets):
    scratch = [pltpu.VMEM((2 * ROWS, 128), jnp.float32)]
    shape = array(BANDS, 2, ROWS, 128)
    return call(apart_kernel, shape, [SMEM, VMEM], scratch, 4, place, targets)


def exchange(*operands):
    scratch = [
        pltpu.VMEM((2, OCC, GRID // 2, 2, 2 * PLANE, 128), jnp.float32),
        pltpu.VMEM((OCC, 2, 2, ROWS, 128), jnp.float32),
    ]
    shape = array(16, FIELD_ROWS + EXTRA, 128, dtype=jnp.bfloat16)
    specs = [SMEM] + [VMEM] * (len(operands) - 1)
    return call(exchange_kernel, shape, specs, scratch, 24, *operands)


def projector(shares):
    return call(projector_kernel, array(256, 128), [VMEM], [], 4, shares)


def interleaved(values):
    tiles = values.reshape(values.shape[0], 2, values.shape[2] // 128, 128)
    return jnp.swapaxes(tiles, 1, 2).reshape(values.shape[0], -1, 128)


def local(targets, partners, pair_map, shifts):
    left, right, twist = (jnp.asarray(table) for table in tables())
    core, group = (lax.axis_index(axis).reshape(1, 1) for axis in ("core", "xh"))
    plane = interleaved(partners[0]).reshape(1, 4 * PLANE, 128)
    operand = jnp.broadcast_to(plane, (PEERS, 4 * PLANE, 128))
    gathered = lax.all_to_all(
        operand, ("xh", "chip"), 0, 0, axis_index_groups=order(PEERS, PLANE_FIRST), tiled=True
    )
    mine = jnp.concatenate([pair_map, shifts[0], group], 1)
    theirs = lax.ppermute(mine, "xh", [(0, 1), (1, 0)])
    parts = apart(group, interleaved(targets[0]))
    gathered, parts = lax.optimization_barrier((gathered, parts))
    swapped = lax.ppermute(gathered, "core", [(0, 1), (1, 0)])
    kernel = prepare(mine, theirs)
    shares = exchange(core, kernel, parts, gathered, swapped, left, right, twist)
    shares = lax.all_to_all(
        shares, ("xh", "zz"), 0, 0, axis_index_groups=order(16, SUM_FIRST), tiled=True
    )
    rows = projector(shares).reshape(2 * BANDS, 16, 2, 128)
    return jnp.swapaxes(rows, 1, 2).reshape(1, 2 * BANDS, 2, 2048)


def solution(mesh):
    split = Mesh(mesh.devices.reshape(16, 2, 2, 8), ("chip", "core", "xh", "zz"))
    ka, pb = ("chip", "core"), ("xh", "zz")
    return jax.shard_map(
        local,
        mesh=split,
        in_specs=(
            P(ka, None, None, None),
            P(pb, None, None, ka),
            P(ka, pb),
            P(ka, pb, None),
        ),
        out_specs=P(ka, None, None, pb),
        check_vma=False,
    )
```

```python
import jax
import jax.numpy as jnp
import numpy as np
from jax import lax
from jax.experimental import pallas as pl
from jax.experimental.pallas import tpu as pltpu
from jax.sharding import Mesh
from jax.sharding import PartitionSpec as P


GRID = 32
BANDS = 4
OCC = 2
OWN = 2
PLANE = 8
ROWS = GRID * PLANE
CELLS = GRID**3
KPOINT_SCALING = 2.0
SCREENING_CUTOFF = 0.25
FIELD_ROWS = 32 * OWN
EXTRA = 8
PEERS = 32
PLANE_FIRST = 21
SUM_FIRST = 14
PAIRS = [(0, 0, 0), (1, 1, 0), (0, 1, 0), (0, 1, 1), (2, 0, 0), (2, 0, 1), (3, 1, 0), (3, 1, 1)]


def phases(angle):
    turn = 2.0 * np.pi * (angle % GRID) / GRID
    return np.cos(turn), np.sin(turn)


def tables():
    row = np.arange(ROWS)
    lane = np.arange(128)
    hi, lo = row // PLANE, row % PLANE
    cos, sin = phases(hi[:, None] * hi[None] + 4 * lo[:, None] * lo[None])
    left = np.block([[cos, sin], [-sin, cos]])
    part, z = lane // GRID, lane % GRID
    cos, sin = phases(z[:, None] * z[None] + 8 * part[:, None] * part[None])
    right = np.block([[cos, -sin], [sin, cos]])
    twist = np.stack(phases(lo[:, None] * part[None]))
    return left.astype(jnp.bfloat16), right.astype(jnp.bfloat16), twist.astype(np.float32)


def wave_number(index):
    return ((index + GRID // 2) % GRID - GRID // 2).astype(jnp.float32)


def coulomb(offset, shift):
    row = lax.broadcasted_iota(jnp.int32, (ROWS, 128), 0)
    lane = lax.broadcasted_iota(jnp.int32, (ROWS, 128), 1)
    index = (row // PLANE, (lane // GRID) * PLANE + row % PLANE, lane % GRID)
    lattice = (offset // 16, offset // 4 % 4, offset % 4)
    squared = jnp.zeros((ROWS, 128), jnp.float32)
    for axis in range(3):
        moved = shift[axis].astype(jnp.float32) + lattice[axis].astype(jnp.float32) * 0.25
        component = wave_number(index[axis]) + moved
        squared += component * component
    return KPOINT_SCALING / (squared + SCREENING_CUTOFF)


def order(count, first):
    return [[at ^ first for at in range(count)]]


def product(a, b):
    return jnp.dot(a, b, preferred_element_type=jnp.float32)


def coulomb_kernel(mine, theirs, kernel):
    place = mine[0, 4]
    for q in range(2):
        number = [jnp.where(place == q, mine[0, at], theirs[0, at]) for at in range(4)]
        kernel[q] = coulomb(number[0], number[1:]) * (1.0 / CELLS)


def apart_kernel(place, targets, parts, rows):
    for slot in range(BANDS):
        rows[...] = targets[band_of(slot, place[0, 0])].astype(jnp.float32)
        for part in range(2):
            parts[slot, part] = rows[pl.ds(part, ROWS, 2), :]


def band_of(slot, place):
    return 2 * place + slot if slot < OWN else slot - (1 + 2 * (slot - OWN)) * place


def exchange_kernel(core, kernel, targets, own, other, left, right, twist, out, rows, parts):
    for source, parity in ((own, core[0, 0]), (other, 1 - core[0, 0])):
        for q in range(2):
            for j in range(OCC):
                for m in range(16):
                    at = (16 * q + m) ^ PLANE_FIRST
                    planes = source[at : at + 1, 16 * j : 16 * j + 16].astype(jnp.float32)
                    rows[q, j, m : m + 1, pl.ds(parity, 1)] = planes[:, None]
    for q in range(2):
        for j in range(OCC):
            for part in range(2):
                parts[j, q, part] = rows[q, j, :, :, pl.ds(part, PLANE, 2), :].reshape(ROWS, 128)

    def twisted(re, im):
        return re * twist[0] + im * twist[1], im * twist[0] - re * twist[1]

    def density(band, j):
        tops, bottoms = [], []
        for q in range(2):
            re, im = parts[j, q, 0], parts[j, q, 1]
            tops.append(re * targets[band, 0] + im * targets[band, 1])
            bottoms.append(re * targets[band, 1] - im * targets[band, 0])
        return joined(tops, bottoms)

    def joined(tops, bottoms):
        rows = [jnp.concatenate(tops, 1), jnp.concatenate(bottoms, 1)]
        return jnp.concatenate(rows, 0).astype(jnp.bfloat16)

    def to_spectrum(blocks):
        pairs = []
        for q in range(2):
            cut = slice(128 * q, 128 * q + 128)
            pair = twisted(blocks[:ROWS, cut], blocks[ROWS:, cut])
            pairs.append(jnp.concatenate(pair, 1).astype(jnp.bfloat16))
        return product(jnp.concatenate(pairs, 0), right[...])

    def from_spectrum(spectrum):
        scaled = []
        for q in range(2):
            cut = slice(ROWS * q, ROWS * q + ROWS)
            pair = spectrum[cut, :128] * kernel[q], spectrum[cut, 128:] * -kernel[q]
            scaled.append(jnp.concatenate(pair, 1).astype(jnp.bfloat16))
        return product(jnp.concatenate(scaled, 0), right[...])

    def untwisted(back):
        tops, bottoms = [], []
        for q in range(2):
            cut = slice(ROWS * q, ROWS * q + ROWS)
            re, im = twisted(back[cut, :128], back[cut, 128:])
            tops.append(re)
            bottoms.append(im)
        return joined(tops, bottoms)

    def field(conjugates):
        re_sum, im_sum = None, None
        for j in range(OCC):
            for q in range(2):
                cut = slice(128 * q, 128 * q + 128)
                re, im = conjugates[j][:ROWS, cut], conjugates[j][ROWS:, cut]
                re_now = -(parts[j, q, 0] * re) - parts[j, q, 1] * im
                im_now = parts[j, q, 0] * im - parts[j, q, 1] * re
                re_sum = re_now if re_sum is None else re_sum + re_now
                im_sum = im_now if im_sum is None else im_sum + im_now
        return re_sum, im_sum

    units = [(band, j) for band in range(OWN) for j in range(OCC)]
    values = [product(left[...], density(*unit)) for unit in units]
    values = [to_spectrum(value) for value in values]
    values = [from_spectrum(value) for value in values]
    values = [product(left[...], untwisted(value)) for value in values]
    sums = {}
    for band in range(OWN):
        re, im = field(values[OCC * band : OCC * band + OCC])
        for part, value in enumerate((re, im)):
            value = value.astype(jnp.bfloat16).reshape(16, 16, 128)
            first = 32 * band + 16 * part
            for to in range(16):
                at = to ^ SUM_FIRST
                out[at : at + 1, first : first + 16] = value[to : to + 1]
        for slot, place, cross in PAIRS:
            if place == band:
                if cross:
                    total = targets[slot, 1] * re - targets[slot, 0] * im
                else:
                    total = targets[slot, 0] * re + targets[slot, 1] * im
                sums[slot, place, cross] = total.reshape(GRID, 8, 128).sum(0)
    value = jnp.concatenate([jnp.sum(sums[key], 0, keepdims=True) for key in PAIRS], 0)
    value = jnp.broadcast_to(jnp.sum(value, 1, keepdims=True), (8, 128))
    piece = lax.broadcasted_iota(jnp.int32, (8, 128), 1) // 32
    high = value.astype(jnp.bfloat16).astype(jnp.float32)
    middle = (value - high).astype(jnp.bfloat16).astype(jnp.float32)
    low = value - high - middle
    value = jnp.where(piece == 0, high, jnp.where(piece == 1, middle, jnp.where(piece == 2, low, 0.0)))
    out[:, FIELD_ROWS:] = jnp.broadcast_to(value.astype(jnp.bfloat16)[None], (16, EXTRA, 128))


def projector_kernel(shares, out):
    totals = []
    for group in range(2):
        total = shares[(8 * group) ^ SUM_FIRST].astype(jnp.float32)
        for source in range(8 * group + 1, 8 * group + 8):
            total += shares[source ^ SUM_FIRST].astype(jnp.float32)
        totals.append(total)
    value = {}
    for group in range(2):
        values = totals[group][FIELD_ROWS:]
        values = values + pltpu.roll(values, 96, 1) + pltpu.roll(values, 64, 1)
        values = values * (1.0 / CELLS)
        for at, (slot, own, cross) in enumerate(PAIRS):
            key = band_of(slot, group), band_of(own, group), cross
            value[key] = jnp.broadcast_to(values[at : at + 1, 0:1], (8, 128))

    def entry(row, column):
        i, j = row % BANDS, column % BANDS
        if row // BANDS == column // BANDS:
            return -(value[i, j, 0] if (i, j, 0) in value else value[j, i, 0])
        if i == j:
            return None
        return value[i, j, 1] if (i, j, 1) in value else -value[j, i, 1]

    size = 2 * BANDS
    factor, inverse = {}, {}
    for column in range(size):
        for row in range(column, size):
            rest = entry(row, column)
            for before in range(column):
                if (row, before) in factor and (column, before) in factor:
                    part = factor[row, before] * factor[column, before]
                    rest = -part if rest is None else rest - part
            if row == column:
                guess = lax.rsqrt(rest)
                inverse[row] = guess * (1.5 - 0.5 * rest * guess * guess)
            elif rest is not None:
                factor[row, column] = rest * inverse[column]
    solved = []
    for row in range(size):
        for_parts = []
        for part in range(2):
            band = row % BANDS
            at = 32 * (band % OWN) + 16 * (part if row < BANDS else 1 - part)
            rest = totals[band // OWN][at : at + 16].reshape(2, 8, 128)
            if row >= BANDS and part == 0:
                rest = -rest
            for before in range(row):
                if (row, before) in factor:
                    rest = rest - factor[row, before][None] * solved[before][part]
            rest = rest * inverse[row][None]
            for_parts.append(rest)
            out[pl.ds(32 * row + part, 16, 2), :] = rest.reshape(16, 128)
        solved.append(for_parts)


SMEM = pl.BlockSpec(memory_space=pltpu.SMEM)
VMEM = pl.BlockSpec(memory_space=pltpu.VMEM)


def call(kernel, shapes, specs, scratch, limit, *operands):
    return pl.pallas_call(
        kernel,
        out_shape=shapes,
        in_specs=specs,
        out_specs=jax.tree.map(lambda _: VMEM, shapes),
        scratch_shapes=scratch,
        compiler_params=pltpu.CompilerParams(vmem_limit_bytes=limit << 20),
    )(*operands)


def array(*shape, dtype=jnp.float32):
    return jax.ShapeDtypeStruct(shape, dtype)


def prepare(mine, theirs):
    return call(coulomb_kernel, array(2, ROWS, 128), [SMEM, SMEM], [], 2, mine, theirs)


def apart(place, targets):
    scratch = [pltpu.VMEM((2 * ROWS, 128), jnp.float32)]
    shape = array(BANDS, 2, ROWS, 128)
    return call(apart_kernel, shape, [SMEM, VMEM], scratch, 4, place, targets)


def exchange(*operands):
    scratch = [
        pltpu.VMEM((2, OCC, GRID // 2, 2, 2 * PLANE, 128), jnp.float32),
        pltpu.VMEM((OCC, 2, 2, ROWS, 128), jnp.float32),
    ]
    shape = array(16, FIELD_ROWS + EXTRA, 128, dtype=jnp.bfloat16)
    specs = [SMEM] + [VMEM] * (len(operands) - 1)
    return call(exchange_kernel, shape, specs, scratch, 24, *operands)


def projector(shares):
    return call(projector_kernel, array(256, 128), [VMEM], [], 4, shares)


def interleaved(values):
    tiles = values.reshape(values.shape[0], 2, values.shape[2] // 128, 128)
    return jnp.swapaxes(tiles, 1, 2).reshape(values.shape[0], -1, 128)


def local(targets, partners, pair_map, shifts):
    left, right, twist = (jnp.asarray(table) for table in tables())
    core, group = (lax.axis_index(axis).reshape(1, 1) for axis in ("core", "xh"))
    plane = interleaved(partners[0]).reshape(1, 4 * PLANE, 128)
    operand = jnp.broadcast_to(plane, (PEERS, 4 * PLANE, 128))
    gathered = lax.all_to_all(
        operand, ("xh", "chip"), 0, 0, axis_index_groups=order(PEERS, PLANE_FIRST), tiled=True
    )
    mine = jnp.concatenate([pair_map, shifts[0], group], 1)
    theirs = lax.ppermute(mine, "xh", [(0, 1), (1, 0)])
    parts = apart(group, interleaved(targets[0]))
    gathered, parts = lax.optimization_barrier((gathered, parts))
    swapped = lax.ppermute(gathered, "core", [(0, 1), (1, 0)])
    kernel = prepare(mine, theirs)
    shares = exchange(core, kernel, parts, gathered, swapped, left, right, twist)
    shares = lax.all_to_all(
        shares, ("xh", "zz"), 0, 0, axis_index_groups=order(16, SUM_FIRST), tiled=True
    )
    rows = projector(shares).reshape(2 * BANDS, 16, 2, 128)
    return jnp.swapaxes(rows, 1, 2).reshape(1, 2 * BANDS, 2, 2048)


def solution(mesh):
    split = Mesh(mesh.devices.reshape(16, 2, 2, 8), ("chip", "core", "xh", "zz"))
    ka, pb = ("chip", "core"), ("xh", "zz")
    return jax.shard_map(
        local,
        mesh=split,
        in_specs=(
            P(ka, None, None, None),
            P(pb, None, None, ka),
            P(ka, pb),
            P(ka, pb, None),
        ),
        out_specs=P(ka, None, None, pb),
        check_vma=False,
    )
```
